512 devices in a mesh: dom: 64 (over x_lo, z, core), orb: 8 (over y, x_hi).
Axes of the slice: x: 4 (x_hi: 2, x_lo: 2; x = x_hi * 2 + x_lo), y: 4, z: 16, core: 2. Of those that a mesh axis runs over, the one named last changes fastest.
Arguments:
- orbitals: bfloat16 [16, 256, 256, 128], P('orb', 'dom'), may hold values from -2.390625 to 2.390625
- energies: float32 [16], P('orb'), may hold values from -1.5 to -0.3
- local_potential: float32 [256, 256, 128], P('dom'), may hold values from -4 to 4
- lanczos: bfloat16 [16, 256, 256, 128], P('orb', 'dom'), may hold values from -40 to 40
- previous: bfloat16 [16, 256, 256, 128], P('orb', 'dom'), may hold values from -6 to 6
- beta: float32 [1], replicated, may hold values from 0.3 to 1.5
Outputs:
- next_vector: bfloat16 [16, 256, 256, 128], P('orb', 'dom')
- alpha: float32 [1], replicated
- beta_next: float32 [1], replicated
The draws below stay inside these ranges and needn't reach their ends.
All inputs are finite; a program needn't handle non-finite values.
Results may differ from the reference program's by a relative error of at most 0.0085.
Values may be sent and summed in bfloat16 or wider, within the bound.
A program may use at most 64 MiB of HBM per device.

```python
import math
import jax
import jax.numpy as jnp
from jax import lax

NX = 256
NY = 256
NZ = 128
ORBITALS = 16


def draw_lanczos(key, part):
    subkeys = jax.random.split(jax.random.fold_in(key, 11), 3)
    orbital_rank = jnp.arange(ORBITALS, dtype=jnp.float32) / max(ORBITALS - 1, 1)
    plane_rank = jnp.arange(NX, dtype=jnp.float32) / (NX - 1)
    orbital_scale = jnp.exp((orbital_rank - 0.5) * jnp.log(3.0) + jax.random.uniform(subkeys[0], (ORBITALS,), minval=-0.6, maxval=0.6))
    plane_scale = jnp.exp((plane_rank - 0.5) * jnp.log(3.0) + jax.random.uniform(subkeys[1], (NX,), minval=-0.35, maxval=0.35))
    values = jnp.clip(jax.random.normal(subkeys[2], (ORBITALS, NX, NY, NZ)), -4.0, 4.0)
    scaled = values * orbital_scale[:, None, None, None] * plane_scale[None, :, None, None]
    return scaled.astype(jnp.bfloat16)


def shard_levels(stream_key, dims, cuts, low, high):
    def one(dim, parts):
        steps = jax.random.uniform(jax.random.fold_in(jax.random.fold_in(stream_key, 6), dim), (parts,), jnp.float32, low / len(cuts), high / len(cuts))
        return jnp.repeat(jnp.exp(steps), dims[dim] // parts).reshape((-1,) + (1,) * (len(dims) - dim - 1))

    level = one(*cuts[0])
    for cut in cuts[1:]:
        level = level * one(*cut)
    return level


def bell_draw(own_key, extent, width, most, cuts=(), held_as=jnp.bfloat16):
    factor_of = shard_levels(own_key, extent, cuts, -0.22, 0.18) if cuts else 1.0
    array = jax.random.normal(own_key, extent, jnp.float32) * width * factor_of
    return jnp.minimum(jnp.maximum(array, -most), most).astype(held_as)


def setup_inputs(seed: int = 0) -> dict:
    key_list = jax.random.split(jax.random.key(seed), 7)
    return {
        "orbitals": bell_draw(key_list[0], (ORBITALS, NX, NY, NZ), 0.4, 2.390625, ((0, 8), (1, 64))),
        "energies": jnp.clip(-1.5 + 1.2 * jax.random.uniform(key_list[1], (ORBITALS,), jnp.float32) ** shard_levels(key_list[1], (ORBITALS,), ((0, 8),), -0.2, 0.2), -1.5, -0.3),
        "local_potential": bell_draw(key_list[2], (NX, NY, NZ), 1.0, 4.0, ((0, 64),), jnp.float32),
        "lanczos": draw_lanczos(jax.random.fold_in(key_list[6], 71), 0),
        "previous": bell_draw(key_list[4], (ORBITALS, NX, NY, NZ), 1.0, 6.0, ((0, 8), (1, 64))),
        "beta": jnp.clip(jnp.exp(jax.random.uniform(key_list[5], (1,), jnp.float32, math.log(0.3), math.log(1.5))), 0.3, 1.5),
    }


side_weights = (1.5, -0.15, 1.0 / 90.0)
central_weight = -49.0 / 18.0
screening = 1.0 / 64.0

def cas_table(length):
    position = jnp.arange(length, dtype=jnp.int32)
    phase = position[:, None] * position[None, :] % length
    angle = 2.0 * jnp.pi / length * phase.astype(jnp.float32)
    return jnp.cos(angle) + jnp.sin(angle)

def wave_square(position, length):
    folded = jnp.minimum(position, length - position).astype(jnp.float32)
    wavenumber = 2.0 * jnp.pi / length * folded
    return wavenumber * wavenumber

def laplacian(values):
    running = 3.0 * central_weight * values
    for dimension in range(3):
        for offset, weight in enumerate(side_weights):
            reach = offset + 1
            running = running + weight * (jnp.roll(values, reach, dimension) + jnp.roll(values, -reach, dimension))
    return running

def transform_all(values):
    highest = lax.Precision.HIGHEST
    result = jnp.einsum('ax,xyz->ayz', cas_table(NX), values, precision=highest)
    result = jnp.einsum('by,ayz->abz', cas_table(NY), result, precision=highest)
    return jnp.einsum('cz,abz->abc', cas_table(NZ), result, precision=highest)

def solve_screened(density):
    square_x = wave_square(jnp.arange(NX, dtype=jnp.int32), NX)
    square_y = wave_square(jnp.arange(NY, dtype=jnp.int32), NY)
    square_z = wave_square(jnp.arange(NZ, dtype=jnp.int32), NZ)
    summed = square_x[:, None, None] + square_y[None, :, None] + square_z[None, None, :] + screening
    kernel_values = 4.0 * jnp.pi / (NX * NY * NZ) / summed
    return transform_all(kernel_values * transform_all(density))

def reference(orbitals, energies, local_potential, lanczos, previous, beta):

    def density_step(running, members):
        return (running + members[0].astype(jnp.float32) * members[1].astype(jnp.float32), None)
    density, _ = lax.scan(density_step, jnp.zeros((NX, NY, NZ), jnp.float32), (orbitals, lanczos))
    potential = solve_screened(density)
    entries = float(ORBITALS * NX * NY * NZ)
    positions = jnp.arange(ORBITALS, dtype=jnp.int32)

    def image_of(position):
        current = lanczos[position].astype(jnp.float32)
        image = -0.5 * laplacian(current) + (local_potential - energies[position]) * current
        return (current, image + orbitals[position].astype(jnp.float32) * potential)

    def correlation(position):
        current, image = image_of(position)
        return jnp.sum(current * image)
    rayleigh = jnp.sum(lax.map(correlation, positions)) / entries
    beta_now = beta[0]

    def remainder_of(position):
        current, image = image_of(position)
        return image - rayleigh * current - beta_now * previous[position].astype(jnp.float32)

    def square_sum(position):
        remainder = remainder_of(position)
        return jnp.sum(remainder * remainder)
    squares = jnp.sum(lax.map(square_sum, positions)) / entries
    norm_next = jnp.sqrt(squares + 1e-06)

    def normalized(position):
        return (remainder_of(position) / norm_next).astype(jnp.bfloat16)
    next_vector = lax.map(normalized, positions)
    return (next_vector, jnp.reshape(rayleigh, (1,)), jnp.reshape(norm_next, (1,)))
```

```python
import functools

import jax
import jax.numpy as jnp
import ml_dtypes
import numpy as np
from jax import lax
from jax.experimental import pallas as pl
from jax.experimental.pallas import tpu as pltpu
from jax.sharding import PartitionSpec as P

side_weights = (1.5, -0.15, 1.0 / 90.0)
central_weight = -49.0 / 18.0
screening = 1.0 / 64.0
MESH = pl.DeviceIdType.MESH
F32 = jnp.float32
BF16 = jnp.bfloat16


def cas_table(length):
    position = np.arange(length)
    angle = 2.0 * np.pi / length * (position[:, None] * position[None, :] % length)
    return np.cos(angle) + np.sin(angle)


def side_table(length, center):
    table = center * np.eye(length)
    for offset, weight in enumerate(side_weights):
        for shift in (offset + 1, -offset - 1):
            table = table + weight * np.roll(np.eye(length), shift, 0)
    return -0.5 * table


def high_low(table):
    high = table.astype(np.float32).astype(ml_dtypes.bfloat16)
    low = (table - high.astype(np.float64)).astype(np.float32).astype(ml_dtypes.bfloat16)
    return [high, low]


def split(value):
    high = value.astype(BF16)
    return high, (value - high.astype(F32)).astype(BF16)


def dot(a, b):
    return jnp.dot(a, b, preferred_element_type=F32)


def dot3(a, b):
    return dot(a[0], b[0]) + (dot(a[0], b[1]) + dot(a[1], b[0]))


def folded_square(position, length):
    folded = jnp.minimum(position, length - position).astype(F32) * (2.0 * np.pi / length)
    return folded * folded


def partner(me, step, size):
    side = lax.rem(step, 2)
    rank = lax.div(step, 2)
    odd = lax.rem(rank, 2)
    delta = odd * lax.div(rank + 1, 2) - (1 - odd) * lax.div(rank, 2)
    return lax.rem(me + size // 4 + side * (size // 2) + delta, size)


def everyone(me, size, action):
    def one(step, carry):
        action(partner(me, step, size))
        return carry

    lax.fori_loop(0, size - 1, one, 0)


def cyclic(me, size, action):
    def one(step, carry):
        action(lax.rem(me + 1 + step, size))
        return carry

    lax.fori_loop(0, size - 1, one, 0)


def wait_bytes(ref, sem):
    pltpu.make_async_copy(ref, ref, sem).wait()


def kernel(
    nd, no, energies, beta, orb_hbm, loc_hbm, cur_hbm, pre_hbm, t128_hbm, ty_hbm, tx_hbm,
    out_hbm, alpha_out, norm_out,
    orb, loc, cur, pre, t128, ty, tx, out, img, below, above,
    rs_send, rs_recv, a_send, a_recv, b_send, b_recv, g_send, g_recv,
    mo_send, mo_recv, md_send, md_recv, early,
    load_sem, near_sem, send_sem, recv_sem, out_sem,
):
    me = lax.axis_index("dom")
    mine = lax.axis_index("orb")
    count, planes, ny, nz = cur.shape
    rows = ny // no
    half = nz // 2
    barrier = pltpu.get_barrier_semaphore()
    everyone(me, nd, lambda j: pl.semaphore_signal(
        barrier, inc=1, device_id={"dom": j}, device_id_type=MESH))
    cyclic(mine, no, lambda j: pl.semaphore_signal(
        barrier, inc=1, device_id={"orb": j}, device_id_type=MESH))

    loads = [
        pltpu.make_async_copy(s, d, load_sem.at[n])
        for n, (s, d) in enumerate((
            (cur_hbm, cur), (orb_hbm, orb), (t128_hbm, t128), (ty_hbm, ty),
            (pre_hbm, pre), (loc_hbm, loc), (tx_hbm, tx),
        ))
    ]
    for load in loads:
        load.start()
    for load in loads[:4]:
        load.wait()
    cz = (t128[0], t128[1])

    def forward(p, carry):
        field = jnp.zeros((ny, nz), F32)
        for i in range(count):
            field = field + orb[i, p].astype(F32) * cur[i, p].astype(F32)
        field = dot3(split(field), cz)
        field = dot3((ty[0], ty[1]), split(field))
        rs_send[:, p] = field.reshape(no, rows, nz).astype(BF16)
        return carry

    lax.fori_loop(0, planes, forward, 0)
    pl.semaphore_wait(barrier, nd + no - 2)

    cyclic(mine, no, lambda j: pltpu.make_async_remote_copy(
        rs_send.at[j], rs_recv.at[mine], send_sem.at[0], recv_sem.at[0],
        device_id={"orb": j}, device_id_type=MESH).start())
    upward = pltpu.make_async_remote_copy(
        cur.at[:, pl.ds(planes - 3, 3)], below, near_sem.at[0], near_sem.at[1],
        device_id={"dom": lax.rem(me + 1, nd)}, device_id_type=MESH)
    downward = pltpu.make_async_remote_copy(
        cur.at[:, pl.ds(0, 3)], above, near_sem.at[2], near_sem.at[3],
        device_id={"dom": lax.rem(me + nd - 1, nd)}, device_id_type=MESH)
    upward.start()
    downward.start()
    rs_recv[mine] = rs_send[mine]

    for load in loads[4:]:
        load.wait()

    def folded(value):
        return jnp.sum(value.reshape(ny // 8, 8, nz), axis=0)

    def local(n, sums):
        i, p = lax.div(n, planes), lax.rem(n, planes)
        here = cur[i, p]
        value = here.astype(F32)
        old = pre[i, p].astype(F32)
        near = dot(ty[2], here) + dot(ty[3], here)
        near = near + dot(here, t128[2]) + dot(here, t128[3])
        img[i, p] = near + (loc[p] - energies[i]) * value
        return (
            sums[0] + folded(value * value),
            sums[1] + folded(value * old),
            sums[2] + folded(old * old),
        )

    zero = jnp.zeros((8, nz), F32)
    known = lax.fori_loop(0, count * planes, local, (zero, zero, zero))
    for n in range(3):
        early[n] = known[n]

    lane = lax.broadcasted_iota(jnp.int32, (rows, nz), 1)
    low = lane < half

    wait_bytes(rs_recv.at[pl.ds(0, no - 1)], recv_sem.at[0])
    s = []
    for p in range(planes):
        total = rs_recv[0, p].astype(F32)
        for o in range(1, no):
            total = total + rs_recv[o, p].astype(F32)
        s.append(total)
    turned = [pltpu.roll(v, half, 1) for v in s]
    for q in range(2):
        a_send[:rows, q, :] = jnp.where(low, s[q], turned[q + 2])
        a_send[rows:, q, :] = jnp.where(low, turned[q], s[q + 2])

    def slot(j):
        return lax.rem(j, 2) * rows + lax.div(j, 2)

    def all_to_all(source, target, n):
        everyone(me, nd, lambda j: pltpu.make_async_remote_copy(
            source.at[slot(j)], target.at[slot(me)], send_sem.at[n], recv_sem.at[n],
            device_id={"dom": j}, device_id_type=MESH).start())
        target[slot(me)] = source[slot(me)]

    all_to_all(a_send, a_recv, 1)

    upward.wait()
    downward.wait()

    def lines(i, carry):
        line = [below[i, p].astype(F32) for p in range(3)]
        line = line + [cur[i, p].astype(F32) for p in range(planes)]
        line = line + [above[i, p].astype(F32) for p in range(3)]
        for p in range(planes):
            value = img[i, p]
            for n, weight in enumerate(side_weights):
                value = value + (-0.5 * weight) * (line[p + 4 + n] + line[p + 2 - n])
            img[i, p] = value
        return carry

    lax.fori_loop(0, count, lines, 0)

    row = mine * rows + lax.div(me, 2)
    column = lax.rem(me, 2) * half + lax.rem(
        lax.broadcasted_iota(jnp.int32, (1, nz), 1), half)
    nx = nd * planes
    kx = folded_square(lax.broadcasted_iota(jnp.int32, (nx, nz), 0), nx)
    ky = folded_square(jnp.full((1, nz), row, jnp.int32), ny)
    weight = (4.0 * np.pi / (nx * ny * nz)) / (kx + (ky + folded_square(column, nz) + screening))
    wide = lax.broadcasted_iota(jnp.int32, (nx, nz), 1) < half

    wait_bytes(a_recv.at[pl.ds(0, nd - 1)], recv_sem.at[1])
    gathered = split(jnp.concatenate([a_recv[:, q, :] for q in range(2)], axis=0))
    size = nx // 2
    first = dot3((tx[0, :, :size], tx[1, :, :size]), gathered)
    second = dot3((tx[0, :, size:], tx[1, :, size:]), gathered)
    modes = jnp.where(
        wide, first + pltpu.roll(second, half, 1), pltpu.roll(first, half, 1) + second)
    modes = split(modes * weight)
    back = dot3((tx[2], tx[3]), modes)
    back = jnp.where(wide[:size], back[:size], back[size:])
    for q in range(2):
        b_send[:, q, :] = back[q * nd : (q + 1) * nd]

    all_to_all(b_send, b_recv, 2)
    wait_bytes(b_recv.at[pl.ds(0, nd - 1)], recv_sem.at[2])
    for q in range(2):
        even, odd = b_recv[:rows, q, :], b_recv[rows:, q, :]
        g_send[q] = jnp.where(low, even, pltpu.roll(odd, half, 1)).astype(BF16)
        g_send[q + 2] = jnp.where(low, pltpu.roll(even, half, 1), odd).astype(BF16)

    cyclic(mine, no, lambda j: pltpu.make_async_remote_copy(
        g_send, g_recv.at[mine], send_sem.at[3], recv_sem.at[3],
        device_id={"orb": j}, device_id_type=MESH).start())
    g_recv[mine] = g_send[...]
    wait_bytes(g_recv.at[pl.ds(0, no - 1)], recv_sem.at[3])

    def finish(p, sums):
        field = g_recv[:, p].reshape(ny, nz)
        field = dot(ty[0], field) + dot(ty[1], field)
        field = dot3(split(field), cz)
        for i in range(count):
            value = img[i, p] + orb[i, p].astype(F32) * field
            img[i, p] = value
            sums = (
                sums[0] + folded(cur[i, p].astype(F32) * value),
                sums[1] + folded(value * value),
                sums[2] + folded(pre[i, p].astype(F32) * value),
            )
        return sums

    late = lax.fori_loop(0, planes, finish, (zero, zero, zero))
    ones = lax.broadcasted_iota(jnp.int32, (1, nz), 1)

    def whole(value):
        return jnp.sum(jnp.sum(value, axis=0, keepdims=True), axis=1, keepdims=True)

    packed = jnp.zeros((1, nz), F32)
    for n, value in enumerate((*late, early[0], early[1], early[2])):
        packed = jnp.where(ones == n, whole(value), packed)
    mo_send[...] = packed
    cyclic(mine, no, lambda j: pltpu.make_async_remote_copy(
        mo_send, mo_recv.at[mine], send_sem.at[4], recv_sem.at[4],
        device_id={"orb": j}, device_id_type=MESH).start())
    mo_recv[mine] = packed
    wait_bytes(mo_recv.at[pl.ds(0, no - 1)], recv_sem.at[4])
    packed = jnp.sum(mo_recv[...], axis=0)
    md_send[...] = packed
    everyone(me, nd, lambda j: pltpu.make_async_remote_copy(
        md_send, md_recv.at[me], send_sem.at[5], recv_sem.at[5],
        device_id={"dom": j}, device_id_type=MESH).start())
    md_recv[me] = packed
    wait_bytes(md_recv.at[pl.ds(0, nd - 1)], recv_sem.at[5])
    packed = jnp.sum(md_recv[...], axis=0) * (1.0 / (count * no * nx * ny * nz))

    cross, image, older_image, own, mixed, older = [
        jnp.sum(jnp.where(ones == n, packed, 0.0), axis=1, keepdims=True) for n in range(6)
    ]
    beta_now = beta[0]
    squares = image - 2.0 * cross * cross - 2.0 * beta_now * older_image
    squares = squares + cross * cross * own + 2.0 * cross * beta_now * mixed
    squares = squares + beta_now * beta_now * older
    norm = jnp.sqrt(squares + 1e-06)
    inverse = 1.0 / norm
    alpha_out[0] = cross[0, 0]
    norm_out[0] = norm[0, 0]

    def scale(n, carry):
        i, p = lax.div(n, planes), lax.rem(n, planes)
        value = img[i, p] - cross * cur[i, p].astype(F32) - beta_now * pre[i, p].astype(F32)
        out[i, p] = (value * inverse).astype(BF16)
        return carry

    lax.fori_loop(0, count * planes, scale, 0)
    store = pltpu.make_async_copy(out, out_hbm, out_sem)
    store.start()
    wait_bytes(rs_send.at[pl.ds(0, no - 1)], send_sem.at[0])
    wait_bytes(a_send.at[pl.ds(0, nd - 1)], send_sem.at[1])
    wait_bytes(b_send.at[pl.ds(0, nd - 1)], send_sem.at[2])
    wait_bytes(g_recv.at[pl.ds(0, no - 1)], send_sem.at[3])
    wait_bytes(mo_recv.at[pl.ds(0, no - 1)], send_sem.at[4])
    wait_bytes(md_recv.at[pl.ds(0, nd - 1)], send_sem.at[5])
    store.wait()


def per_device(nd, no, orbitals, energies, local_potential, lanczos, previous, beta):
    count, planes, ny, nz = lanczos.shape
    rows, nx = ny // no, nd * planes
    order = np.array([
        planes * (2 * r + h) + 2 * lane_half + q
        for lane_half in range(2) for q in range(2) for h in range(2) for r in range(rows)
    ])
    cas_x = cas_table(nx)
    t128 = np.stack(high_low(cas_table(nz)) + high_low(side_table(nz, central_weight)))
    ty = np.stack(high_low(cas_table(ny)) + high_low(side_table(ny, 2.0 * central_weight)))
    tx = np.stack(high_low(cas_x[:, order]) + high_low(cas_x[order, :]))
    hbm = pl.BlockSpec(memory_space=pl.ANY)
    smem = pl.BlockSpec(memory_space=pltpu.SMEM)
    vmem = pltpu.VMEM
    field = (count, planes, ny, nz)
    dma = pltpu.SemaphoreType.DMA
    return pl.pallas_call(
        functools.partial(kernel, nd, no),
        out_shape=(
            jax.ShapeDtypeStruct(field, BF16),
            jax.ShapeDtypeStruct((1,), F32),
            jax.ShapeDtypeStruct((1,), F32),
        ),
        in_specs=[smem, smem] + [hbm] * 7,
        out_specs=(hbm, smem, smem),
        scratch_shapes=[
            vmem(field, BF16), vmem(field[1:], F32), vmem(field, BF16), vmem(field, BF16),
            vmem(t128.shape, BF16), vmem(ty.shape, BF16), vmem(tx.shape, BF16),
            vmem(field, BF16), vmem(field, F32),
            vmem((count, 3, ny, nz), BF16), vmem((count, 3, ny, nz), BF16),
            vmem((no, planes, rows, nz), BF16), vmem((no, planes, rows, nz), BF16),
            vmem((nd, 2, nz), F32), vmem((nd, 2, nz), F32),
            vmem((nd, 2, nz), F32), vmem((nd, 2, nz), F32),
            vmem((planes, rows, nz), BF16), vmem((no, planes, rows, nz), BF16),
            vmem((1, nz), F32), vmem((no, 1, nz), F32),
            vmem((1, nz), F32), vmem((nd, 1, nz), F32),
            vmem((3, 8, nz), F32),
            dma((7,)), dma((4,)), dma((6,)), dma((6,)), dma(()),
        ],
        compiler_params=pltpu.CompilerParams(collective_id=0, has_side_effects=True),
    )(energies, beta, orbitals, local_potential, lanczos, previous,
      jnp.asarray(t128), jnp.asarray(ty), jnp.asarray(tx))


def solution(mesh):
    placed = (
        P("orb", "dom", None, None),
        P("orb"),
        P("dom", None, None),
        P("orb", "dom", None, None),
        P("orb", "dom", None, None),
        P(),
    )
    return jax.shard_map(
        functools.partial(per_device, mesh.shape["dom"], mesh.shape["orb"]),
        mesh=mesh,
        in_specs=placed,
        out_specs=(P("orb", "dom", None, None), P(), P()),
        check_vma=False,
    )
```

```python
import functools

import jax
import jax.numpy as jnp
import ml_dtypes
import numpy as np
from jax import lax
from jax.experimental import pallas as pl
from jax.experimental.pallas import tpu as pltpu
from jax.sharding import PartitionSpec as P

side_weights = (1.5, -0.15, 1.0 / 90.0)
central_weight = -49.0 / 18.0
screening = 1.0 / 64.0
MESH = pl.DeviceIdType.MESH
F32 = jnp.float32
BF16 = jnp.bfloat16


def cas_table(length):
    position = np.arange(length)
    angle = 2.0 * np.pi / length * (position[:, None] * position[None, :] % length)
    return np.cos(angle) + np.sin(angle)


def side_table(length, center):
    table = center * np.eye(length)
    for offset, weight in enumerate(side_weights):
        for shift in (offset + 1, -offset - 1):
            table = table + weight * np.roll(np.eye(length), shift, 0)
    return -0.5 * table


def high_low(table):
    high = table.astype(np.float32).astype(ml_dtypes.bfloat16)
    low = (table - high.astype(np.float64)).astype(np.float32).astype(ml_dtypes.bfloat16)
    return [high, low]


def split(value):
    high = value.astype(BF16)
    return high, (value - high.astype(F32)).astype(BF16)


def dot(a, b):
    return jnp.dot(a, b, preferred_element_type=F32)


def dot3(a, b):
    return dot(a[0], b[0]) + (dot(a[0], b[1]) + dot(a[1], b[0]))


def folded_square(position, length):
    folded = jnp.minimum(position, length - position).astype(F32) * (2.0 * np.pi / length)
    return folded * folded


def everyone(me, size, action):
    quarter = size // 4
    around = lambda offset: action(lax.rem(me + offset, size))
    around(quarter)
    around(3 * quarter)

    def nearer(step, carry):
        around(quarter + step)
        around(quarter - step)
        around(3 * quarter + step)
        around(3 * quarter - step)
        return carry

    lax.fori_loop(1, quarter, nearer, 0)
    around(2 * quarter)


def cyclic(me, size, action):
    for step in range(1, size):
        action(lax.rem(me + step, size))


def wait_bytes(ref, sem):
    pltpu.make_async_copy(ref, ref, sem).wait()


def kernel(
    nd, no, energies_hbm, beta_hbm, orb_hbm, loc_hbm, cur_hbm, pre_hbm, t128_hbm, ty_hbm, tx_hbm,
    out, alpha_out, norm_out,
    orb, loc, cur, pre, t128, ty, tx, img, below, above,
    rs_send, rs_recv, a_send, a_recv, b_send, b_recv, g_send, g_recv,
    mo_send, mo_recv, md_send, md_recv, early, stage, energies, beta,
    load_sem, near_sem, send_sem, recv_sem, plane_sem,
):
    me = lax.axis_index("dom")
    mine = lax.axis_index("orb")
    count, planes, ny, nz = cur.shape
    rows = ny // no
    half = nz // 2
    loads = [
        pltpu.make_async_copy(s, d, load_sem.at[n])
        for n, (s, d) in enumerate((
            (cur_hbm, cur), (orb_hbm, orb), (t128_hbm, t128), (ty_hbm, ty),
            (pre_hbm, pre), (loc_hbm, loc), (tx_hbm, tx),
            (energies_hbm, energies), (beta_hbm, beta),
        ))
    ]
    for load in loads:
        load.start()
    barrier = pltpu.get_barrier_semaphore()
    everyone(me, nd, lambda j: pl.semaphore_signal(
        barrier, inc=1, device_id={"dom": j}, device_id_type=MESH))
    cyclic(mine, no, lambda j: pl.semaphore_signal(
        barrier, inc=1, device_id={"orb": j}, device_id_type=MESH))

    for load in loads[:4]:
        load.wait()
    cz = (t128[0], t128[1])

    def forward(p, carry):
        field = jnp.zeros((ny, nz), F32)
        for i in range(count):
            field = field + orb[i, p].astype(F32) * cur[i, p].astype(F32)
        field = dot3(split(field), cz)
        field = dot3((ty[0], ty[1]), split(field))
        rs_send[:, p] = field.reshape(no, rows, nz).astype(BF16)
        return carry

    lax.fori_loop(0, planes, forward, 0)
    pl.semaphore_wait(barrier, nd + no - 2)

    cyclic(mine, no, lambda j: pltpu.make_async_remote_copy(
        rs_send.at[j], rs_recv.at[mine], send_sem.at[0], recv_sem.at[0],
        device_id={"orb": j}, device_id_type=MESH).start())
    upward = pltpu.make_async_remote_copy(
        cur.at[:, pl.ds(planes - 3, 3)], below, near_sem.at[0], near_sem.at[1],
        device_id={"dom": lax.rem(me + 1, nd)}, device_id_type=MESH)
    downward = pltpu.make_async_remote_copy(
        cur.at[:, pl.ds(0, 3)], above, near_sem.at[2], near_sem.at[3],
        device_id={"dom": lax.rem(me + nd - 1, nd)}, device_id_type=MESH)
    turn = nd // 2
    top = lax.rem(me, turn) == turn - 1
    bottom = lax.rem(me, turn) == 0

    @pl.when(jnp.logical_not(top))
    def _():
        upward.start()

    @pl.when(jnp.logical_not(bottom))
    def _():
        downward.start()

    rs_recv[mine] = rs_send[mine]

    for load in loads[4:]:
        load.wait()

    def folded(value):
        return jnp.sum(value.reshape(ny // 8, 8, nz), axis=0)

    def local(n, sums):
        i, p = lax.div(n, planes), lax.rem(n, planes)
        here = cur[i, p]
        value = here.astype(F32)
        old = pre[i, p].astype(F32)
        near = dot(ty[2], here) + dot(ty[3], here)
        near = near + dot(here, t128[2]) + dot(here, t128[3])
        img[i, p] = near + (loc[p] - energies[i]) * value
        return (
            sums[0] + folded(value * value),
            sums[1] + folded(value * old),
            sums[2] + folded(old * old),
        )

    zero = jnp.zeros((8, nz), F32)
    known = lax.fori_loop(0, count * planes, local, (zero, zero, zero))
    for n in range(3):
        early[n] = known[n]

    lane = lax.broadcasted_iota(jnp.int32, (rows, nz), 1)
    low = lane < half

    wait_bytes(rs_recv.at[pl.ds(0, no - 1)], recv_sem.at[0])
    s = []
    for p in range(planes):
        total = rs_recv[0, p].astype(F32)
        for o in range(1, no):
            total = total + rs_recv[o, p].astype(F32)
        s.append(total)
    turned = [pltpu.roll(v, half, 1) for v in s]
    for q in range(2):
        stage[:rows, q, :] = jnp.where(low, s[q], turned[q + 2])
        stage[rows:, q, :] = jnp.where(low, turned[q], s[q + 2])
    a_send[...] = stage[...].astype(BF16)

    def slot(j):
        return lax.rem(j, 2) * rows + lax.div(j, 2)

    def all_to_all(source, target, n):
        everyone(me, nd, lambda j: pltpu.make_async_remote_copy(
            source.at[slot(j)], target.at[slot(me)], send_sem.at[n], recv_sem.at[n],
            device_id={"dom": j}, device_id_type=MESH).start())
        target[slot(me)] = source[slot(me)]

    all_to_all(a_send, a_recv, 1)

    @pl.when(top)
    def _():
        upward.start()

    @pl.when(bottom)
    def _():
        downward.start()

    row = mine * rows + lax.div(me, 2)
    column = lax.rem(me, 2) * half + lax.rem(
        lax.broadcasted_iota(jnp.int32, (1, nz), 1), half)
    nx = nd * planes
    kx = folded_square(lax.broadcasted_iota(jnp.int32, (nx, nz), 0), nx)
    ky = folded_square(jnp.full((1, nz), row, jnp.int32), ny)
    weight = (4.0 * np.pi / (nx * ny * nz)) / (kx + (ky + folded_square(column, nz) + screening))
    wide = lax.broadcasted_iota(jnp.int32, (nx, nz), 1) < half

    wait_bytes(a_recv.at[pl.ds(0, nd - 1)], recv_sem.at[1])
    stage[...] = a_recv[...].astype(F32)
    gathered = jnp.concatenate([stage[:, q, :] for q in range(2)], axis=0).astype(BF16)
    size = nx // 2
    first = dot(tx[0, :, :size], gathered) + dot(tx[1, :, :size], gathered)
    second = dot(tx[0, :, size:], gathered) + dot(tx[1, :, size:], gathered)
    modes = jnp.where(
        wide, first + pltpu.roll(second, half, 1), pltpu.roll(first, half, 1) + second)
    modes = split(modes * weight)
    back = dot3((tx[2], tx[3]), modes)
    back = jnp.where(wide[:size], back[:size], back[size:])
    for q in range(2):
        stage[:, q, :] = back[q * nd : (q + 1) * nd]
    b_send[...] = stage[...].astype(BF16)

    all_to_all(b_send, b_recv, 2)
    upward.wait()
    downward.wait()

    def lines(i, carry):
        line = [below[i, p].astype(F32) for p in range(3)]
        line = line + [cur[i, p].astype(F32) for p in range(planes)]
        line = line + [above[i, p].astype(F32) for p in range(3)]
        for p in range(planes):
            value = img[i, p]
            for n, weight in enumerate(side_weights):
                value = value + (-0.5 * weight) * (line[p + 4 + n] + line[p + 2 - n])
            img[i, p] = value
        return carry

    lax.fori_loop(0, count, lines, 0)

    wait_bytes(b_recv.at[pl.ds(0, nd - 1)], recv_sem.at[2])
    stage[...] = b_recv[...].astype(F32)
    for q in range(2):
        even, odd = stage[:rows, q, :], stage[rows:, q, :]
        g_send[q] = jnp.where(low, even, pltpu.roll(odd, half, 1)).astype(BF16)
        g_send[q + 2] = jnp.where(low, pltpu.roll(even, half, 1), odd).astype(BF16)

    for p in range(planes):
        cyclic(mine, no, lambda j: pltpu.make_async_remote_copy(
            g_send.at[p], g_recv.at[mine, p], send_sem.at[3], plane_sem.at[p],
            device_id={"orb": j}, device_id_type=MESH).start())
    g_recv[mine] = g_send[...]

    def finish(p, sums):
        wait_bytes(g_recv.at[pl.ds(0, no - 1), p], plane_sem.at[p])
        field = g_recv[:, p].reshape(ny, nz)
        field = dot(ty[0], field) + dot(ty[1], field)
        field = dot3(split(field), cz)
        for i in range(count):
            value = img[i, p] + orb[i, p].astype(F32) * field
            img[i, p] = value
            sums = (
                sums[0] + folded(cur[i, p].astype(F32) * value),
                sums[1] + folded(value * value),
                sums[2] + folded(pre[i, p].astype(F32) * value),
            )
        return sums

    late = lax.fori_loop(0, planes, finish, (zero, zero, zero))
    ones = lax.broadcasted_iota(jnp.int32, (1, nz), 1)

    def whole(value):
        return jnp.sum(jnp.sum(value, axis=0, keepdims=True), axis=1, keepdims=True)

    packed = jnp.zeros((1, nz), F32)
    for n, value in enumerate((*late, early[0], early[1], early[2])):
        packed = jnp.where(ones == n, whole(value), packed)
    mo_send[...] = packed
    cyclic(mine, no, lambda j: pltpu.make_async_remote_copy(
        mo_send, mo_recv.at[mine], send_sem.at[4], recv_sem.at[4],
        device_id={"orb": j}, device_id_type=MESH).start())
    mo_recv[mine] = packed
    wait_bytes(mo_recv.at[pl.ds(0, no - 1)], recv_sem.at[4])
    packed = jnp.sum(mo_recv[...], axis=0)
    md_send[...] = packed
    everyone(me, nd, lambda j: pltpu.make_async_remote_copy(
        md_send, md_recv.at[me], send_sem.at[5], recv_sem.at[5],
        device_id={"dom": j}, device_id_type=MESH).start())
    md_recv[me] = packed
    wait_bytes(md_recv.at[pl.ds(0, nd - 1)], recv_sem.at[5])
    packed = jnp.sum(md_recv[...], axis=0) * (1.0 / (count * no * nx * ny * nz))

    cross, image, older_image, own, mixed, older = [
        jnp.sum(jnp.where(ones == n, packed, 0.0), axis=1, keepdims=True) for n in range(6)
    ]
    beta_now = beta[0]
    squares = image - 2.0 * cross * cross - 2.0 * beta_now * older_image
    squares = squares + cross * cross * own + 2.0 * cross * beta_now * mixed
    squares = squares + beta_now * beta_now * older
    norm = jnp.sqrt(squares + 1e-06)
    inverse = 1.0 / norm
    alpha_out[0] = cross[0, 0]
    norm_out[0] = norm[0, 0]

    def scale(n, carry):
        i, p = lax.div(n, planes), lax.rem(n, planes)
        value = img[i, p] - cross * cur[i, p].astype(F32) - beta_now * pre[i, p].astype(F32)
        out[i, p] = (value * inverse).astype(BF16)
        return carry

    lax.fori_loop(0, count * planes, scale, 0)
    wait_bytes(rs_send.at[pl.ds(0, no - 1)], send_sem.at[0])
    wait_bytes(a_send.at[pl.ds(0, nd - 1)], send_sem.at[1])
    wait_bytes(b_send.at[pl.ds(0, nd - 1)], send_sem.at[2])
    wait_bytes(g_recv.at[pl.ds(0, no - 1)], send_sem.at[3])
    wait_bytes(mo_recv.at[pl.ds(0, no - 1)], send_sem.at[4])
    wait_bytes(md_recv.at[pl.ds(0, nd - 1)], send_sem.at[5])


def per_device(nd, no, orbitals, energies, local_potential, lanczos, previous, beta):
    count, planes, ny, nz = lanczos.shape
    rows, nx = ny // no, nd * planes
    order = np.array([
        planes * (2 * r + h) + 2 * lane_half + q
        for lane_half in range(2) for q in range(2) for h in range(2) for r in range(rows)
    ])
    cas_x = cas_table(nx)
    t128 = np.stack(high_low(cas_table(nz)) + high_low(side_table(nz, central_weight)))
    ty = np.stack(high_low(cas_table(ny)) + high_low(side_table(ny, 2.0 * central_weight)))
    tx = np.stack(high_low(cas_x[:, order]) + high_low(cas_x[order, :]))
    hbm = pl.BlockSpec(memory_space=pl.ANY)
    smem = pl.BlockSpec(memory_space=pltpu.SMEM)
    vmem = pltpu.VMEM
    field = (count, planes, ny, nz)
    dma = pltpu.SemaphoreType.DMA
    return pl.pallas_call(
        functools.partial(kernel, nd, no),
        out_shape=(
            pltpu.VMEM(field, BF16),
            jax.ShapeDtypeStruct((1,), F32),
            jax.ShapeDtypeStruct((1,), F32),
        ),
        in_specs=[hbm] * 9,
        out_specs=(pl.BlockSpec(memory_space=vmem), smem, smem),
        scratch_shapes=[
            vmem(field, BF16), vmem(field[1:], F32), vmem(field, BF16), vmem(field, BF16),
            vmem(t128.shape, BF16), vmem(ty.shape, BF16), vmem(tx.shape, BF16),
            vmem(field, F32),
            vmem((count, 3, ny, nz), BF16), vmem((count, 3, ny, nz), BF16),
            vmem((no, planes, rows, nz), BF16), vmem((no, planes, rows, nz), BF16),
            vmem((nd, 2, nz), BF16), vmem((nd, 2, nz), BF16),
            vmem((nd, 2, nz), BF16), vmem((nd, 2, nz), BF16),
            vmem((planes, rows, nz), BF16), vmem((no, planes, rows, nz), BF16),
            vmem((1, nz), F32), vmem((no, 1, nz), F32),
            vmem((1, nz), F32), vmem((nd, 1, nz), F32),
            vmem((3, 8, nz), F32), vmem((nd, 2, nz), F32),
            pltpu.SMEM((count,), F32), pltpu.SMEM((1,), F32),
            dma((9,)), dma((4,)), dma((6,)), dma((6,)), dma((planes,)),
        ],
        compiler_params=pltpu.CompilerParams(collective_id=0, has_side_effects=True),
    )(energies, beta, orbitals, local_potential, lanczos, previous,
      jnp.asarray(t128), jnp.asarray(ty), jnp.asarray(tx))


def solution(mesh):
    placed = (
        P("orb", "dom", None, None),
        P("orb"),
        P("dom", None, None),
        P("orb", "dom", None, None),
        P("orb", "dom", None, None),
        P(),
    )
    return jax.shard_map(
        functools.partial(per_device, mesh.shape["dom"], mesh.shape["orb"]),
        mesh=mesh,
        in_specs=placed,
        out_specs=(P("orb", "dom", None, None), P(), P()),
        check_vma=False,
    )
```

```python
import functools

import jax
import jax.numpy as jnp
import ml_dtypes
import numpy as np
from jax import lax
from jax.experimental import pallas as pl
from jax.experimental.pallas import tpu as pltpu
from jax.sharding import PartitionSpec as P

side_weights = (1.5, -0.15, 1.0 / 90.0)
central_weight = -49.0 / 18.0
screening = 1.0 / 64.0
MESH = pl.DeviceIdType.MESH
F32 = jnp.float32
BF16 = jnp.bfloat16


def cas_table(length):
    position = np.arange(length)
    angle = 2.0 * np.pi / length * (position[:, None] * position[None, :] % length)
    return np.cos(angle) + np.sin(angle)


def side_table(length, center):
    table = center * np.eye(length)
    for offset, weight in enumerate(side_weights):
        for shift in (offset + 1, -offset - 1):
            table = table + weight * np.roll(np.eye(length), shift, 0)
    return -0.5 * table


def high_low(table):
    high = table.astype(np.float32).astype(ml_dtypes.bfloat16)
    low = (table - high.astype(np.float64)).astype(np.float32).astype(ml_dtypes.bfloat16)
    return [high, low]


def split(value):
    high = value.astype(BF16)
    return high, (value - high.astype(F32)).astype(BF16)


def dot(a, b):
    return jnp.dot(a, b, preferred_element_type=F32)


def dot3(a, b):
    return dot(a[0], b[0]) + (dot(a[0], b[1]) + dot(a[1], b[0]))


def folded_square(position, length):
    folded = jnp.minimum(position, length - position).astype(F32) * (2.0 * np.pi / length)
    return folded * folded


def everyone(me, size, action):
    quarter = size // 4
    around = lambda offset: action(lax.rem(me + offset, size))
    around(quarter)
    around(3 * quarter)

    def nearer(step, carry):
        around(quarter + step)
        around(quarter - step)
        around(3 * quarter + step)
        around(3 * quarter - step)
        return carry

    lax.fori_loop(1, quarter, nearer, 0)
    around(2 * quarter)


def cyclic(me, size, action):
    for step in range(1, size):
        action(lax.rem(me + step, size))


def wait_bytes(ref, sem):
    pltpu.make_async_copy(ref, ref, sem).wait()


def kernel(
    nd, no, energies_hbm, beta_hbm, orb_hbm, loc_hbm, cur_hbm, pre_hbm, t128_hbm, ty_hbm, tx_hbm,
    out, alpha_out, norm_out,
    orb, loc, cur, pre, t128, ty, tx, img, below, above,
    rs_send, rs_recv, a_send, a_recv, b_send, b_recv, g_send, g_recv,
    mo_send, mo_recv, md_send, md_recv, early, stage, mixed_fields, potential, energies, beta,
    load_sem, near_sem, send_sem, recv_sem, plane_sem, heard, all_heard,
):
    me = lax.axis_index("dom")
    mine = lax.axis_index("orb")
    count, planes, ny, nz = cur.shape
    rows = ny // no
    half = nz // 2
    loads = [
        pltpu.make_async_copy(s, d, load_sem.at[n])
        for n, (s, d) in enumerate((
            (cur_hbm, cur), (orb_hbm, orb), (t128_hbm, t128), (ty_hbm, ty),
            (pre_hbm, pre), (loc_hbm, loc), (tx_hbm, tx),
            (energies_hbm, energies), (beta_hbm, beta),
        ))
    ]
    for load in loads:
        load.start()
    ring = nd // 4
    core = lax.rem(me, 2)
    wide_x = lax.div(me, nd // 2)
    depth = lax.rem(lax.div(me, 2), ring)

    def along(offset):
        return wide_x * (nd // 2) + lax.rem(depth + offset + ring, ring) * 2 + core

    def beside(a, b):
        return lax.rem(wide_x + a, 2) * (nd // 2) + depth * 2 + lax.rem(core + b, 2)

    outer = lax.rem(me + 2 * core - 1 + nd, nd)
    chips = ((1, 1), (1, 0), (0, 1))

    def tell(sem, j):
        pl.semaphore_signal(sem, inc=1, device_id={"dom": j}, device_id_type=MESH)

    barrier = pltpu.get_barrier_semaphore()
    cyclic(mine, no, lambda j: pl.semaphore_signal(
        barrier, inc=1, device_id={"orb": j}, device_id_type=MESH))
    for j in [beside(*c) for c in chips] + [along(1), along(-1), outer]:
        tell(barrier, j)

    for load in loads[:4]:
        load.wait()
    cz = (t128[0], t128[1])

    def forward(p, carry):
        field = jnp.zeros((ny, nz), F32)
        for i in range(count):
            field = field + orb[i, p].astype(F32) * cur[i, p].astype(F32)
        field = dot3(split(field), cz)
        field = dot3((ty[0], ty[1]), split(field))
        rs_send[:, p] = field.reshape(no, rows, nz).astype(BF16)
        return carry

    def spread(n, stride):
        tell(heard.at[n], along(stride))
        tell(heard.at[n], along(-stride))

    strides = [1]
    while 2 * sum(strides, 1) < ring:
        strides.append(sum(strides, 1))
    def scatter(p):
        cyclic(mine, no, lambda j: pltpu.make_async_remote_copy(
            rs_send.at[j, p], rs_recv.at[mine, p], send_sem.at[0], recv_sem.at[0],
            device_id={"orb": j}, device_id_type=MESH).start())

    first = planes // 2
    lax.fori_loop(0, first, forward, 0)
    pl.semaphore_wait(barrier, no + 5)
    spread(0, strides[0])
    for p in range(first):
        scatter(p)
    for p in range(first, planes):
        forward(p, 0)
        scatter(p)
    upward = pltpu.make_async_remote_copy(
        cur.at[:, pl.ds(planes - 3, 3)], below, near_sem.at[0], near_sem.at[1],
        device_id={"dom": lax.rem(me + 1, nd)}, device_id_type=MESH)
    downward = pltpu.make_async_remote_copy(
        cur.at[:, pl.ds(0, 3)], above, near_sem.at[2], near_sem.at[3],
        device_id={"dom": lax.rem(me + nd - 1, nd)}, device_id_type=MESH)
    turn = nd // 2
    top = lax.rem(me, turn) == turn - 1
    bottom = lax.rem(me, turn) == 0

    @pl.when(jnp.logical_not(top))
    def _():
        upward.start()

    @pl.when(jnp.logical_not(bottom))
    def _():
        downward.start()

    rs_recv[mine] = rs_send[mine]

    for load in loads[4:]:
        load.wait()

    def folded(value):
        return jnp.sum(value.reshape(ny // 8, 8, nz), axis=0)

    def local(n, sums):
        i, p = lax.div(n, planes), lax.rem(n, planes)
        here = cur[i, p]
        value = here.astype(F32)
        old = pre[i, p].astype(F32)
        near = dot(ty[2], here) + dot(ty[3], here)
        near = near + dot(here, t128[2]) + dot(here, t128[3])
        img[i, p] = near + (loc[p] - energies[i]) * value
        return (
            sums[0] + folded(value * value),
            sums[1] + folded(value * old),
            sums[2] + folded(old * old),
        )

    zero = jnp.zeros((8, nz), F32)
    known = (zero, zero, zero)
    piece = count * planes // len(strides)
    for n in range(len(strides)):
        stop = count * planes if n == len(strides) - 1 else (n + 1) * piece
        known = lax.fori_loop(n * piece, stop, local, known)
        pl.semaphore_wait(heard.at[n], 2)
        if n + 1 < len(strides):
            spread(n + 1, strides[n + 1])
    for c in chips:
        tell(all_heard, beside(*c))
    for n in range(3):
        early[n] = known[n]

    lane = lax.broadcasted_iota(jnp.int32, (rows, nz), 1)
    low = lane < half

    wait_bytes(rs_recv.at[pl.ds(0, no - 1)], recv_sem.at[0])
    s = []
    for p in range(planes):
        total = rs_recv[0, p].astype(F32)
        for o in range(1, no):
            total = total + rs_recv[o, p].astype(F32)
        s.append(total)
    turned = [pltpu.roll(v, half, 1) for v in s]
    for q in range(2):
        stage[:rows, q, :] = jnp.where(low, s[q], turned[q + 2])
        stage[rows:, q, :] = jnp.where(low, turned[q], s[q + 2])
    a_send[...] = stage[...].astype(BF16)

    def slot(j):
        return lax.rem(j, 2) * rows + lax.div(j, 2)

    def all_to_all(source, target, n):
        everyone(me, nd, lambda j: pltpu.make_async_remote_copy(
            source.at[slot(j)], target.at[slot(me)], send_sem.at[n], recv_sem.at[n],
            device_id={"dom": j}, device_id_type=MESH).start())
        target[slot(me)] = source[slot(me)]

    pl.semaphore_wait(all_heard, 3)
    all_to_all(a_send, a_recv, 1)

    @pl.when(top)
    def _():
        upward.start()

    @pl.when(bottom)
    def _():
        downward.start()

    row = mine * rows + lax.div(me, 2)
    column = lax.rem(me, 2) * half + lax.rem(
        lax.broadcasted_iota(jnp.int32, (1, nz), 1), half)
    nx = nd * planes
    kx = folded_square(lax.broadcasted_iota(jnp.int32, (nx, nz), 0), nx)
    ky = folded_square(jnp.full((1, nz), row, jnp.int32), ny)
    weight = (4.0 * np.pi / (nx * ny * nz)) / (kx + (ky + folded_square(column, nz) + screening))
    wide = lax.broadcasted_iota(jnp.int32, (nx, nz), 1) < half

    wait_bytes(a_recv.at[pl.ds(0, nd - 1)], recv_sem.at[1])
    stage[...] = a_recv[...].astype(F32)
    gathered = jnp.concatenate([stage[:, q, :] for q in range(2)], axis=0).astype(BF16)
    size = nx // 2
    first = dot(tx[0, :, :size], gathered) + dot(tx[1, :, :size], gathered)
    second = dot(tx[0, :, size:], gathered) + dot(tx[1, :, size:], gathered)
    modes = jnp.where(
        wide, first + pltpu.roll(second, half, 1), pltpu.roll(first, half, 1) + second)
    modes = split(modes * weight)
    back = dot3((tx[2], tx[3]), modes)
    back = jnp.where(wide[:size], back[:size], back[size:])
    for q in range(2):
        stage[:, q, :] = back[q * nd : (q + 1) * nd]
    b_send[...] = stage[...].astype(BF16)

    all_to_all(b_send, b_recv, 2)
    upward.wait()
    downward.wait()

    def lines(i, carry):
        line = [below[i, p].astype(F32) for p in range(3)]
        line = line + [cur[i, p].astype(F32) for p in range(planes)]
        line = line + [above[i, p].astype(F32) for p in range(3)]
        for p in range(planes):
            value = img[i, p]
            for n, weight in enumerate(side_weights):
                value = value + (-0.5 * weight) * (line[p + 4 + n] + line[p + 2 - n])
            img[i, p] = value
        return carry

    lax.fori_loop(0, count, lines, 0)

    def prepare(p, sums):
        pair = jnp.zeros((ny, nz), F32)
        aged, based, square = pair, pair, pair
        for i in range(count):
            base, weight_o = img[i, p], orb[i, p].astype(F32)
            value, old = cur[i, p].astype(F32), pre[i, p].astype(F32)
            pair = pair + weight_o * value
            aged = aged + weight_o * old
            based = based + weight_o * base
            square = square + weight_o * weight_o
            sums = (
                sums[0] + folded(value * base),
                sums[1] + folded(base * base),
                sums[2] + folded(old * base),
            )
        for n, field in enumerate((pair, aged, 2.0 * based, square)):
            mixed_fields[n, p] = field
        return sums

    based = lax.fori_loop(0, planes, prepare, (zero, zero, zero))
    for n in range(3):
        early[3 + n] = based[n]

    wait_bytes(b_recv.at[pl.ds(0, nd - 1)], recv_sem.at[2])
    stage[...] = b_recv[...].astype(F32)
    for q in range(2):
        even, odd = stage[:rows, q, :], stage[rows:, q, :]
        g_send[q] = jnp.where(low, even, pltpu.roll(odd, half, 1)).astype(BF16)
        g_send[q + 2] = jnp.where(low, pltpu.roll(even, half, 1), odd).astype(BF16)

    for p in range(planes):
        cyclic(mine, no, lambda j: pltpu.make_async_remote_copy(
            g_send.at[p], g_recv.at[mine, p], send_sem.at[3], plane_sem.at[p],
            device_id={"orb": j}, device_id_type=MESH).start())
    g_recv[mine] = g_send[...]

    def finish(p, sums):
        wait_bytes(g_recv.at[pl.ds(0, no - 1), p], plane_sem.at[p])
        field = g_recv[:, p].reshape(ny, nz)
        field = dot(ty[0], field) + dot(ty[1], field)
        field = dot3(split(field), cz)
        potential[p] = field
        return (
            sums[0] + folded(mixed_fields[0, p] * field),
            sums[1] + folded((mixed_fields[2, p] + mixed_fields[3, p] * field) * field),
            sums[2] + folded(mixed_fields[1, p] * field),
        )

    late = lax.fori_loop(0, planes, finish, (early[3], early[4], early[5]))
    ones = lax.broadcasted_iota(jnp.int32, (1, nz), 1)

    def whole(value):
        return jnp.sum(jnp.sum(value, axis=0, keepdims=True), axis=1, keepdims=True)

    packed = jnp.zeros((1, nz), F32)
    for n, value in enumerate((*late, early[0], early[1], early[2])):
        packed = jnp.where(ones == n, whole(value), packed)
    mo_send[...] = packed
    here = mine * 4 + wide_x * 2 + core
    for step in range(no):
        for c in chips + ((0, 0),):
            if step or c != (0, 0):
                pltpu.make_async_remote_copy(
                    mo_send, mo_recv.at[here], send_sem.at[4], recv_sem.at[4],
                    device_id={"dom": beside(*c), "orb": lax.rem(mine + step, no)},
                    device_id_type=MESH).start()
    mo_recv[here] = packed
    wait_bytes(mo_recv.at[pl.ds(0, 4 * no - 1)], recv_sem.at[4])
    packed = jnp.sum(mo_recv[...], axis=0)
    md_send[...] = packed
    for step in sorted(range(1, ring), key=lambda n: abs(2 * n - ring)):
        pltpu.make_async_remote_copy(
            md_send, md_recv.at[depth], send_sem.at[5], recv_sem.at[5],
            device_id={"dom": along(step)}, device_id_type=MESH).start()
    md_recv[depth] = packed
    wait_bytes(md_recv.at[pl.ds(0, ring - 1)], recv_sem.at[5])
    packed = jnp.sum(md_recv[...], axis=0) * (1.0 / (count * no * nx * ny * nz))

    cross, image, older_image, own, mixed, older = [
        jnp.sum(jnp.where(ones == n, packed, 0.0), axis=1, keepdims=True) for n in range(6)
    ]
    beta_now = beta[0]
    squares = image - 2.0 * cross * cross - 2.0 * beta_now * older_image
    squares = squares + cross * cross * own + 2.0 * cross * beta_now * mixed
    squares = squares + beta_now * beta_now * older
    norm = jnp.sqrt(squares + 1e-06)
    inverse = 1.0 / norm
    alpha_out[0] = cross[0, 0]
    norm_out[0] = norm[0, 0]

    def scale(n, carry):
        i, p = lax.div(n, planes), lax.rem(n, planes)
        value = img[i, p] + orb[i, p].astype(F32) * potential[p]
        value = value - cross * cur[i, p].astype(F32) - beta_now * pre[i, p].astype(F32)
        out[i, p] = (value * inverse).astype(BF16)
        return carry

    lax.fori_loop(0, count * planes, scale, 0)
    wait_bytes(rs_send.at[pl.ds(0, no - 1)], send_sem.at[0])
    wait_bytes(a_send.at[pl.ds(0, nd - 1)], send_sem.at[1])
    wait_bytes(b_send.at[pl.ds(0, nd - 1)], send_sem.at[2])
    wait_bytes(g_recv.at[pl.ds(0, no - 1)], send_sem.at[3])
    wait_bytes(mo_recv.at[pl.ds(0, 4 * no - 1)], send_sem.at[4])
    wait_bytes(md_recv.at[pl.ds(0, ring - 1)], send_sem.at[5])


def per_device(nd, no, orbitals, energies, local_potential, lanczos, previous, beta):
    count, planes, ny, nz = lanczos.shape
    rows, nx = ny // no, nd * planes
    order = np.array([
        planes * (2 * r + h) + 2 * lane_half + q
        for lane_half in range(2) for q in range(2) for h in range(2) for r in range(rows)
    ])
    cas_x = cas_table(nx)
    t128 = np.stack(high_low(cas_table(nz)) + high_low(side_table(nz, central_weight)))
    ty = np.stack(high_low(cas_table(ny)) + high_low(side_table(ny, 2.0 * central_weight)))
    tx = np.stack(high_low(cas_x[:, order]) + high_low(cas_x[order, :]))
    hbm = pl.BlockSpec(memory_space=pl.ANY)
    smem = pl.BlockSpec(memory_space=pltpu.SMEM)
    vmem = pltpu.VMEM
    field = (count, planes, ny, nz)
    dma = pltpu.SemaphoreType.DMA
    return pl.pallas_call(
        functools.partial(kernel, nd, no),
        out_shape=(
            pltpu.VMEM(field, BF16),
            jax.ShapeDtypeStruct((1,), F32),
            jax.ShapeDtypeStruct((1,), F32),
        ),
        in_specs=[hbm] * 9,
        out_specs=(pl.BlockSpec(memory_space=vmem), smem, smem),
        scratch_shapes=[
            vmem(field, BF16), vmem(field[1:], F32), vmem(field, BF16), vmem(field, BF16),
            vmem(t128.shape, BF16), vmem(ty.shape, BF16), vmem(tx.shape, BF16),
            vmem(field, F32),
            vmem((count, 3, ny, nz), BF16), vmem((count, 3, ny, nz), BF16),
            vmem((no, planes, rows, nz), BF16), vmem((no, planes, rows, nz), BF16),
            vmem((nd, 2, nz), BF16), vmem((nd, 2, nz), BF16),
            vmem((nd, 2, nz), BF16), vmem((nd, 2, nz), BF16),
            vmem((planes, rows, nz), BF16), vmem((no, planes, rows, nz), BF16),
            vmem((1, nz), F32), vmem((4 * no, 1, nz), F32),
            vmem((1, nz), F32), vmem((nd // 4, 1, nz), F32),
            vmem((6, 8, nz), F32), vmem((nd, 2, nz), F32),
            vmem((4, *field[1:]), F32), vmem(field[1:], F32),
            pltpu.SMEM((count,), F32), pltpu.SMEM((1,), F32),
            dma((9,)), dma((4,)), dma((6,)), dma((6,)), dma((planes,)),
            pltpu.SemaphoreType.REGULAR((4,)), pltpu.SemaphoreType.REGULAR(()),
        ],
        compiler_params=pltpu.CompilerParams(collective_id=0, has_side_effects=True),
    )(energies, beta, orbitals, local_potential, lanczos, previous,
      jnp.asarray(t128), jnp.asarray(ty), jnp.asarray(tx))


def solution(mesh):
    placed = (
        P("orb", "dom", None, None),
        P("orb"),
        P("dom", None, None),
        P("orb", "dom", None, None),
        P("orb", "dom", None, None),
        P(),
    )
    return jax.shard_map(
        functools.partial(per_device, mesh.shape["dom"], mesh.shape["orb"]),
        mesh=mesh,
        in_specs=placed,
        out_specs=(P("orb", "dom", None, None), P(), P()),
        check_vma=False,
    )
```

```python
import functools

import jax
import jax.numpy as jnp
import ml_dtypes
import numpy as np
from jax import lax
from jax.experimental import pallas as pl
from jax.experimental.pallas import tpu as pltpu
from jax.sharding import PartitionSpec as P

side_weights = (1.5, -0.15, 1.0 / 90.0)
central_weight = -49.0 / 18.0
screening = 1.0 / 64.0
MESH = pl.DeviceIdType.MESH
F32 = jnp.float32
BF16 = jnp.bfloat16


def cas_table(length):
    position = np.arange(length)
    angle = 2.0 * np.pi / length * (position[:, None] * position[None, :] % length)
    return np.cos(angle) + np.sin(angle)


def side_table(length, center):
    table = center * np.eye(length)
    for offset, weight in enumerate(side_weights):
        for shift in (offset + 1, -offset - 1):
            table = table + weight * np.roll(np.eye(length), shift, 0)
    return -0.5 * table


def high_low(table):
    high = table.astype(np.float32).astype(ml_dtypes.bfloat16)
    low = (table - high.astype(np.float64)).astype(np.float32).astype(ml_dtypes.bfloat16)
    return [high, low]


def split(value):
    high = value.astype(BF16)
    return high, (value - high.astype(F32)).astype(BF16)


def dot(a, b):
    return jnp.dot(a, b, preferred_element_type=F32)


def dot3(a, b):
    return dot(a[0], b[0]) + (dot(a[0], b[1]) + dot(a[1], b[0]))


def folded_square(position, length):
    folded = jnp.minimum(position, length - position).astype(F32) * (2.0 * np.pi / length)
    return folded * folded


def everyone(me, size, action):
    quarter = size // 4
    around = lambda offset: action(lax.rem(me + offset, size))
    around(quarter)
    around(3 * quarter)

    def nearer(step, carry):
        around(quarter + step)
        around(quarter - step)
        around(3 * quarter + step)
        around(3 * quarter - step)
        return carry

    lax.fori_loop(1, quarter, nearer, 0)
    around(2 * quarter)


def cyclic(me, size, action):
    for step in range(1, size):
        action(lax.rem(me + step, size))


def wait_bytes(ref, sem):
    pltpu.make_async_copy(ref, ref, sem).wait()


def kernel(
    nd, no, energies_hbm, beta_hbm, orb_hbm, loc_hbm, cur_hbm, pre_hbm, t128_hbm, ty_hbm, tx_hbm,
    out, alpha_out, norm_out,
    orb, loc, cur, pre, t128, ty, tx, img, below, above,
    rs_send, rs_recv, a_send, a_recv, b_send, b_recv, g_send, g_recv,
    mo_send, mo_recv, md_send, md_recv, early, stage, mixed_fields, potential, energies, beta,
    load_sem, near_sem, send_sem, recv_sem, plane_sem, heard, all_heard,
):
    me = lax.axis_index("dom")
    mine = lax.axis_index("orb")
    count, planes, ny, nz = cur.shape
    rows = ny // no
    half = nz // 2
    loads = [
        pltpu.make_async_copy(s, d, load_sem.at[n])
        for n, (s, d) in enumerate((
            (cur_hbm, cur), (orb_hbm, orb), (t128_hbm, t128), (ty_hbm, ty),
            (pre_hbm, pre), (loc_hbm, loc), (tx_hbm, tx),
            (energies_hbm, energies), (beta_hbm, beta),
        ))
    ]
    for load in loads:
        load.start()
    ring = nd // 4
    core = lax.rem(me, 2)
    wide_x = lax.div(me, nd // 2)
    depth = lax.rem(lax.div(me, 2), ring)

    def along(offset):
        return wide_x * (nd // 2) + lax.rem(depth + offset + ring, ring) * 2 + core

    def beside(a, b):
        return lax.rem(wide_x + a, 2) * (nd // 2) + depth * 2 + lax.rem(core + b, 2)

    outer = lax.rem(me + 2 * core - 1 + nd, nd)
    chips = ((1, 1), (1, 0), (0, 1))

    def tell(sem, j):
        pl.semaphore_signal(sem, inc=1, device_id={"dom": j}, device_id_type=MESH)

    barrier = pltpu.get_barrier_semaphore()
    cyclic(mine, no, lambda j: pl.semaphore_signal(
        barrier, inc=1, device_id={"orb": j}, device_id_type=MESH))
    for j in [beside(*c) for c in chips] + [along(1), along(-1), outer]:
        tell(barrier, j)

    for load in loads[:4]:
        load.wait()
    cz = (t128[0], t128[1])

    def across(fields):
        return jnp.concatenate(fields, axis=1)

    def stacked(field):
        return jnp.concatenate([field[:, :nz], field[:, nz:]], axis=0)

    def forward(p):
        fields = []
        for n in range(2):
            field = jnp.zeros((ny, nz), F32)
            for i in range(count):
                field = field + orb[i, p + n].astype(F32) * cur[i, p + n].astype(F32)
            fields.append(field)
        field = dot3(split(jnp.concatenate(fields, axis=0)), cz)
        field = dot3((ty[0], ty[1]), split(across([field[:ny], field[ny:]])))
        for n in range(2):
            part = field[:, n * nz : (n + 1) * nz]
            rs_send[:, p + n] = part.reshape(no, rows, nz).astype(BF16)

    def spread(n, stride):
        tell(heard.at[n], along(stride))
        tell(heard.at[n], along(-stride))

    strides = [1]
    while 2 * sum(strides, 1) < ring:
        strides.append(sum(strides, 1))
    def scatter(p):
        cyclic(mine, no, lambda j: pltpu.make_async_remote_copy(
            rs_send.at[j, p], rs_recv.at[mine, p], send_sem.at[0], recv_sem.at[0],
            device_id={"orb": j}, device_id_type=MESH).start())

    for p in range(0, planes, 2):
        forward(p)
        if p == 0:
            pl.semaphore_wait(barrier, no + 5)
            spread(0, strides[0])
        scatter(p)
        scatter(p + 1)
    upward = pltpu.make_async_remote_copy(
        cur.at[:, pl.ds(planes - 3, 3)], below, near_sem.at[0], near_sem.at[1],
        device_id={"dom": lax.rem(me + 1, nd)}, device_id_type=MESH)
    downward = pltpu.make_async_remote_copy(
        cur.at[:, pl.ds(0, 3)], above, near_sem.at[2], near_sem.at[3],
        device_id={"dom": lax.rem(me + nd - 1, nd)}, device_id_type=MESH)
    turn = nd // 2
    top = lax.rem(me, turn) == turn - 1
    bottom = lax.rem(me, turn) == 0

    def inner_halo():
        @pl.when(jnp.logical_not(top))
        def _():
            upward.start()

        @pl.when(jnp.logical_not(bottom))
        def _():
            downward.start()

    rs_recv[mine] = rs_send[mine]

    for load in loads[4:]:
        load.wait()

    def folded(value):
        return jnp.sum(value.reshape(ny // 8, 8, nz), axis=0)

    def local(n, sums):
        i, p = lax.div(n, planes), lax.rem(n, planes)
        here = cur[i, p]
        value = here.astype(F32)
        old = pre[i, p].astype(F32)
        near = dot(ty[2], here) + dot(ty[3], here)
        near = near + dot(here, t128[2]) + dot(here, t128[3])
        img[i, p] = near + (loc[p] - energies[i]) * value
        return (
            sums[0] + folded(value * value),
            sums[1] + folded(value * old),
            sums[2] + folded(old * old),
        )

    zero = jnp.zeros((8, nz), F32)
    known = (zero, zero, zero)
    piece = count * planes // len(strides)
    for n in range(len(strides)):
        stop = count * planes if n == len(strides) - 1 else (n + 1) * piece
        known = lax.fori_loop(n * piece, stop, local, known)
        pl.semaphore_wait(heard.at[n], 2)
        if n + 1 < len(strides):
            spread(n + 1, strides[n + 1])
        if n == max(0, len(strides) - 2):
            inner_halo()
    for c in chips:
        tell(all_heard, beside(*c))
    for n in range(3):
        early[n] = known[n]

    lane = lax.broadcasted_iota(jnp.int32, (rows, nz), 1)
    low = lane < half

    wait_bytes(rs_recv.at[pl.ds(0, no - 1)], recv_sem.at[0])
    s = []
    for p in range(planes):
        total = rs_recv[0, p].astype(F32)
        for o in range(1, no):
            total = total + rs_recv[o, p].astype(F32)
        s.append(total)
    turned = [pltpu.roll(v, half, 1) for v in s]
    for q in range(2):
        stage[:rows, q, :] = jnp.where(low, s[q], turned[q + 2])
        stage[rows:, q, :] = jnp.where(low, turned[q], s[q + 2])
    a_send[...] = stage[...].astype(BF16)

    def slot(j):
        return lax.rem(j, 2) * rows + lax.div(j, 2)

    def all_to_all(source, target, n):
        everyone(me, nd, lambda j: pltpu.make_async_remote_copy(
            source.at[slot(j)], target.at[slot(me)], send_sem.at[n], recv_sem.at[n],
            device_id={"dom": j}, device_id_type=MESH).start())
        target[slot(me)] = source[slot(me)]

    pl.semaphore_wait(all_heard, 3)
    all_to_all(a_send, a_recv, 1)

    @pl.when(top)
    def _():
        upward.start()

    @pl.when(bottom)
    def _():
        downward.start()

    row = mine * rows + lax.div(me, 2)
    column = lax.rem(me, 2) * half + lax.rem(
        lax.broadcasted_iota(jnp.int32, (1, nz), 1), half)
    nx = nd * planes
    kx = folded_square(lax.broadcasted_iota(jnp.int32, (nx, nz), 0), nx)
    ky = folded_square(jnp.full((1, nz), row, jnp.int32), ny)
    weight = (4.0 * np.pi / (nx * ny * nz)) / (kx + (ky + folded_square(column, nz) + screening))
    wide = lax.broadcasted_iota(jnp.int32, (nx, nz), 1) < half

    wait_bytes(a_recv.at[pl.ds(0, nd - 1)], recv_sem.at[1])
    stage[...] = a_recv[...].astype(F32)
    gathered = jnp.concatenate([stage[:, q, :] for q in range(2)], axis=0).astype(BF16)
    size = nx // 2
    first = dot(tx[0, :, :size], gathered) + dot(tx[1, :, :size], gathered)
    second = dot(tx[0, :, size:], gathered) + dot(tx[1, :, size:], gathered)
    modes = jnp.where(
        wide, first + pltpu.roll(second, half, 1), pltpu.roll(first, half, 1) + second)
    modes = split(modes * weight)
    back = dot3((tx[2], tx[3]), modes)
    back = jnp.where(wide[:size], back[:size], back[size:])
    for q in range(2):
        stage[:, q, :] = back[q * nd : (q + 1) * nd]
    b_send[...] = stage[...].astype(BF16)

    all_to_all(b_send, b_recv, 2)
    upward.wait()
    downward.wait()

    def lines(i, carry):
        line = [below[i, p].astype(F32) for p in range(3)]
        line = line + [cur[i, p].astype(F32) for p in range(planes)]
        line = line + [above[i, p].astype(F32) for p in range(3)]
        for p in range(planes):
            value = img[i, p]
            for n, weight in enumerate(side_weights):
                value = value + (-0.5 * weight) * (line[p + 4 + n] + line[p + 2 - n])
            img[i, p] = value
        return carry

    lax.fori_loop(0, count, lines, 0)

    def prepare(p, sums):
        pair = jnp.zeros((ny, nz), F32)
        aged, based, square = pair, pair, pair
        for i in range(count):
            base, weight_o = img[i, p], orb[i, p].astype(F32)
            value, old = cur[i, p].astype(F32), pre[i, p].astype(F32)
            pair = pair + weight_o * value
            aged = aged + weight_o * old
            based = based + weight_o * base
            square = square + weight_o * weight_o
            sums = (
                sums[0] + folded(value * base),
                sums[1] + folded(base * base),
                sums[2] + folded(old * base),
            )
        for n, field in enumerate((pair, aged, 2.0 * based, square)):
            mixed_fields[n, p] = field
        return sums

    based = lax.fori_loop(0, planes, prepare, (zero, zero, zero))
    for n in range(3):
        early[3 + n] = based[n]

    wait_bytes(b_recv.at[pl.ds(0, nd - 1)], recv_sem.at[2])
    stage[...] = b_recv[...].astype(F32)
    for q in range(2):
        even, odd = stage[:rows, q, :], stage[rows:, q, :]
        g_send[q] = jnp.where(low, even, pltpu.roll(odd, half, 1)).astype(BF16)
        g_send[q + 2] = jnp.where(low, pltpu.roll(even, half, 1), odd).astype(BF16)

    for p in range(planes):
        cyclic(mine, no, lambda j: pltpu.make_async_remote_copy(
            g_send.at[p], g_recv.at[mine, p], send_sem.at[3], plane_sem.at[p],
            device_id={"orb": j}, device_id_type=MESH).start())
    g_recv[mine] = g_send[...]

    late = (early[3], early[4], early[5])
    for p in range(0, planes, 2):
        for n in range(2):
            wait_bytes(g_recv.at[pl.ds(0, no - 1), p + n], plane_sem.at[p + n])
        field = across([g_recv[:, p + n].reshape(ny, nz) for n in range(2)])
        field = dot(ty[0], field) + dot(ty[1], field)
        field = dot3(split(stacked(field)), cz)
        for n in range(2):
            part = field[n * ny : (n + 1) * ny]
            potential[p + n] = part
            late = (
                late[0] + folded(mixed_fields[0, p + n] * part),
                late[1] + folded((mixed_fields[2, p + n] + mixed_fields[3, p + n] * part) * part),
                late[2] + folded(mixed_fields[1, p + n] * part),
            )

    ones = lax.broadcasted_iota(jnp.int32, (1, nz), 1)

    def whole(value):
        return jnp.sum(jnp.sum(value, axis=0, keepdims=True), axis=1, keepdims=True)

    packed = jnp.zeros((1, nz), F32)
    for n, value in enumerate((*late, early[0], early[1], early[2])):
        packed = jnp.where(ones == n, whole(value), packed)
    mo_send[...] = packed
    here = mine * 4 + wide_x * 2 + core
    for step in range(no):
        for c in chips + ((0, 0),):
            if step or c != (0, 0):
                pltpu.make_async_remote_copy(
                    mo_send, mo_recv.at[here], send_sem.at[4], recv_sem.at[4],
                    device_id={"dom": beside(*c), "orb": lax.rem(mine + step, no)},
                    device_id_type=MESH).start()
    mo_recv[here] = packed
    wait_bytes(mo_recv.at[pl.ds(0, 4 * no - 1)], recv_sem.at[4])
    packed = jnp.sum(mo_recv[...], axis=0)
    md_send[...] = packed
    for step in sorted(range(1, ring), key=lambda n: abs(2 * n - ring)):
        pltpu.make_async_remote_copy(
            md_send, md_recv.at[depth], send_sem.at[5], recv_sem.at[5],
            device_id={"dom": along(step)}, device_id_type=MESH).start()
    md_recv[depth] = packed
    wait_bytes(md_recv.at[pl.ds(0, ring - 1)], recv_sem.at[5])
    packed = jnp.sum(md_recv[...], axis=0) * (1.0 / (count * no * nx * ny * nz))

    cross, image, older_image, own, mixed, older = [
        jnp.sum(jnp.where(ones == n, packed, 0.0), axis=1, keepdims=True) for n in range(6)
    ]
    beta_now = beta[0]
    squares = image - 2.0 * cross * cross - 2.0 * beta_now * older_image
    squares = squares + cross * cross * own + 2.0 * cross * beta_now * mixed
    squares = squares + beta_now * beta_now * older
    norm = jnp.sqrt(squares + 1e-06)
    inverse = 1.0 / norm
    alpha_out[0] = cross[0, 0]
    norm_out[0] = norm[0, 0]

    def scale(n, carry):
        i, p = lax.div(n, planes), lax.rem(n, planes)
        value = img[i, p] + orb[i, p].astype(F32) * potential[p]
        value = value - cross * cur[i, p].astype(F32) - beta_now * pre[i, p].astype(F32)
        out[i, p] = (value * inverse).astype(BF16)
        return carry

    lax.fori_loop(0, count * planes, scale, 0)
    wait_bytes(rs_send.at[pl.ds(0, no - 1)], send_sem.at[0])
    wait_bytes(a_send.at[pl.ds(0, nd - 1)], send_sem.at[1])
    wait_bytes(b_send.at[pl.ds(0, nd - 1)], send_sem.at[2])
    wait_bytes(g_recv.at[pl.ds(0, no - 1)], send_sem.at[3])
    wait_bytes(mo_recv.at[pl.ds(0, 4 * no - 1)], send_sem.at[4])
    wait_bytes(md_recv.at[pl.ds(0, ring - 1)], send_sem.at[5])


def per_device(nd, no, orbitals, energies, local_potential, lanczos, previous, beta):
    count, planes, ny, nz = lanczos.shape
    rows, nx = ny // no, nd * planes
    order = np.array([
        planes * (2 * r + h) + 2 * lane_half + q
        for lane_half in range(2) for q in range(2) for h in range(2) for r in range(rows)
    ])
    cas_x = cas_table(nx)
    t128 = np.stack(high_low(cas_table(nz)) + high_low(side_table(nz, central_weight)))
    ty = np.stack(high_low(cas_table(ny)) + high_low(side_table(ny, 2.0 * central_weight)))
    tx = np.stack(high_low(cas_x[:, order]) + high_low(cas_x[order, :]))
    smem = pl.BlockSpec(memory_space=pltpu.SMEM)
    vmem = pltpu.VMEM
    field = (count, planes, ny, nz)
    dma = pltpu.SemaphoreType.DMA
    return pl.pallas_call(
        functools.partial(kernel, nd, no),
        out_shape=(
            pltpu.VMEM(field, BF16),
            pltpu.SMEM((1,), F32),
            pltpu.SMEM((1,), F32),
        ),
        in_specs=[pl.BlockSpec(memory_space=pltpu.HBM)] * 9,
        out_specs=(pl.BlockSpec(memory_space=vmem), smem, smem),
        scratch_shapes=[
            vmem(field, BF16), vmem(field[1:], F32), vmem(field, BF16), vmem(field, BF16),
            vmem(t128.shape, BF16), vmem(ty.shape, BF16), vmem(tx.shape, BF16),
            vmem(field, F32),
            vmem((count, 3, ny, nz), BF16), vmem((count, 3, ny, nz), BF16),
            vmem((no, planes, rows, nz), BF16), vmem((no, planes, rows, nz), BF16),
            vmem((nd, 2, nz), BF16), vmem((nd, 2, nz), BF16),
            vmem((nd, 2, nz), BF16), vmem((nd, 2, nz), BF16),
            vmem((planes, rows, nz), BF16), vmem((no, planes, rows, nz), BF16),
            vmem((1, nz), F32), vmem((4 * no, 1, nz), F32),
            vmem((1, nz), F32), vmem((nd // 4, 1, nz), F32),
            vmem((6, 8, nz), F32), vmem((nd, 2, nz), F32),
            vmem((4, *field[1:]), F32), vmem(field[1:], F32),
            pltpu.SMEM((count,), F32), pltpu.SMEM((1,), F32),
            dma((9,)), dma((4,)), dma((6,)), dma((6,)), dma((planes,)),
            pltpu.SemaphoreType.REGULAR((4,)), pltpu.SemaphoreType.REGULAR(()),
        ],
        compiler_params=pltpu.CompilerParams(collective_id=0, has_side_effects=True),
    )(energies, beta, orbitals, local_potential, lanczos, previous,
      jnp.asarray(t128), jnp.asarray(ty), jnp.asarray(tx))


def solution(mesh):
    placed = (
        P("orb", "dom", None, None),
        P("orb"),
        P("dom", None, None),
        P("orb", "dom", None, None),
        P("orb", "dom", None, None),
        P(),
    )
    return jax.shard_map(
        functools.partial(per_device, mesh.shape["dom"], mesh.shape["orb"]),
        mesh=mesh,
        in_specs=placed,
        out_specs=(P("orb", "dom", None, None), P(), P()),
        check_vma=False,
    )
```

```python
import functools

import jax
import jax.numpy as jnp
import ml_dtypes
import numpy as np
from jax import lax
from jax.experimental import pallas as pl
from jax.experimental.pallas import tpu as pltpu
from jax.sharding import PartitionSpec as P

side_weights = (1.5, -0.15, 1.0 / 90.0)
central_weight = -49.0 / 18.0
screening = 1.0 / 64.0
MESH = pl.DeviceIdType.MESH
F32 = jnp.float32
BF16 = jnp.bfloat16


def cas_table(length):
    position = np.arange(length)
    angle = 2.0 * np.pi / length * (position[:, None] * position[None, :] % length)
    return np.cos(angle) + np.sin(angle)


def side_table(length, center):
    table = center * np.eye(length)
    for offset, weight in enumerate(side_weights):
        for shift in (offset + 1, -offset - 1):
            table = table + weight * np.roll(np.eye(length), shift, 0)
    return -0.5 * table


def high_low(table):
    high = table.astype(np.float32).astype(ml_dtypes.bfloat16)
    low = (table - high.astype(np.float64)).astype(np.float32).astype(ml_dtypes.bfloat16)
    return [high, low]


def split(value):
    high = value.astype(BF16)
    return high, (value - high.astype(F32)).astype(BF16)


def dot(a, b):
    return jnp.dot(a, b, preferred_element_type=F32)


def dot3(a, b):
    return dot(a[0], b[0]) + (dot(a[0], b[1]) + dot(a[1], b[0]))


def folded_square(position, length):
    folded = jnp.minimum(position, length - position).astype(F32) * (2.0 * np.pi / length)
    return folded * folded


def everyone(me, size, action):
    quarter = size // 4
    around = lambda offset: action(lax.rem(me + offset, size))
    around(quarter)
    around(3 * quarter)

    def nearer(step, carry):
        around(quarter + step)
        around(quarter - step)
        around(3 * quarter + step)
        around(3 * quarter - step)
        return carry

    lax.fori_loop(1, quarter, nearer, 0)
    around(2 * quarter)


def cyclic(me, size, action):
    for step in range(1, size):
        action(lax.rem(me + step, size))


def wait_bytes(ref, sem):
    pltpu.make_async_copy(ref, ref, sem).wait()


def kernel(
    nd, no, energies_hbm, beta_hbm, orb_hbm, loc_hbm, cur_hbm, pre_hbm, t128_hbm, ty_hbm, tx_hbm,
    out, alpha_out, norm_out,
    orb, loc, cur, pre, t128, ty, tx, img, below, above,
    rs_send, rs_recv, a_send, a_recv, b_send, b_recv, g_send, g_recv,
    mo_send, mo_recv, md_send, md_recv, early, stage, mixed_fields, potential, energies, beta,
    load_sem, near_sem, send_sem, recv_sem, plane_sem, heard, all_heard,
):
    me = lax.axis_index("dom")
    mine = lax.axis_index("orb")
    count, planes, ny, nz = cur.shape
    rows = ny // no
    half = nz // 2
    loads = [
        pltpu.make_async_copy(s, d, load_sem.at[n])
        for n, (s, d) in enumerate((
            (cur_hbm, cur), (orb_hbm, orb), (t128_hbm, t128), (ty_hbm, ty),
            (pre_hbm, pre), (loc_hbm, loc), (tx_hbm, tx),
            (energies_hbm, energies), (beta_hbm, beta),
        ))
    ]
    for load in loads[:4]:
        load.start()
    ring = nd // 4
    core = lax.rem(me, 2)
    wide_x = lax.div(me, nd // 2)
    depth = lax.rem(lax.div(me, 2), ring)

    def along(offset):
        return wide_x * (nd // 2) + lax.rem(depth + offset + ring, ring) * 2 + core

    def beside(a, b):
        return lax.rem(wide_x + a, 2) * (nd // 2) + depth * 2 + lax.rem(core + b, 2)

    outer = lax.rem(me + 2 * core - 1 + nd, nd)
    chips = ((1, 1), (1, 0), (0, 1))

    def tell(sem, j):
        pl.semaphore_signal(sem, inc=1, device_id={"dom": j}, device_id_type=MESH)

    barrier = pltpu.get_barrier_semaphore()
    cyclic(mine, no, lambda j: pl.semaphore_signal(
        barrier, inc=1, device_id={"orb": j}, device_id_type=MESH))
    near = ring // 4
    for step in range(near, 0, -1):
        tell(barrier, along(step))
        tell(barrier, along(-step))
    for j in [beside(*c) for c in chips] + [outer]:
        tell(barrier, j)

    for load in loads[:4]:
        load.wait()
    for load in loads[4:]:
        load.start()
    cz = (t128[0], t128[1])

    def across(fields):
        return jnp.concatenate(fields, axis=1)

    def stacked(field):
        return jnp.concatenate([field[:, :nz], field[:, nz:]], axis=0)

    def forward(p):
        fields = []
        for n in range(2):
            field = jnp.zeros((ny, nz), F32)
            for i in range(count):
                field = field + orb[i, p + n].astype(F32) * cur[i, p + n].astype(F32)
            fields.append(field)
        field = dot3(split(jnp.concatenate(fields, axis=0)), cz)
        field = dot3((ty[0], ty[1]), split(across([field[:ny], field[ny:]])))
        for n in range(2):
            part = field[:, n * nz : (n + 1) * nz]
            rs_send[:, p + n] = part.reshape(no, rows, nz).astype(BF16)

    def scatter(p):
        cyclic(mine, no, lambda j: pltpu.make_async_remote_copy(
            rs_send.at[j, p], rs_recv.at[mine, p], send_sem.at[0], recv_sem.at[0],
            device_id={"orb": j}, device_id_type=MESH).start())

    for p in range(0, planes, 2):
        forward(p)
        if p == 0:
            pl.semaphore_wait(barrier, no + 3 + 2 * near)
            tell(heard, along(near))
            tell(heard, along(-near))
        scatter(p)
        scatter(p + 1)
    upward = pltpu.make_async_remote_copy(
        cur.at[:, pl.ds(planes - 3, 3)], below, near_sem.at[0], near_sem.at[1],
        device_id={"dom": lax.rem(me + 1, nd)}, device_id_type=MESH)
    downward = pltpu.make_async_remote_copy(
        cur.at[:, pl.ds(0, 3)], above, near_sem.at[2], near_sem.at[3],
        device_id={"dom": lax.rem(me + nd - 1, nd)}, device_id_type=MESH)
    turn = nd // 2
    top = lax.rem(me, turn) == turn - 1
    bottom = lax.rem(me, turn) == 0

    @pl.when(jnp.logical_not(top))
    def _():
        upward.start()

    @pl.when(jnp.logical_not(bottom))
    def _():
        downward.start()

    rs_recv[mine] = rs_send[mine]

    for load in loads[4:]:
        load.wait()

    def folded(value):
        return jnp.sum(value.reshape(ny // 8, 8, nz), axis=0)

    def local(n, sums):
        i, p = lax.div(n, planes), lax.rem(n, planes)
        here = cur[i, p]
        value = here.astype(F32)
        old = pre[i, p].astype(F32)
        near = dot(ty[2], here) + dot(ty[3], here)
        near = near + dot(here, t128[2]) + dot(here, t128[3])
        img[i, p] = near + (loc[p] - energies[i]) * value
        return (
            sums[0] + folded(value * value),
            sums[1] + folded(value * old),
            sums[2] + folded(old * old),
        )

    zero = jnp.zeros((8, nz), F32)
    known = lax.fori_loop(0, count * planes, local, (zero, zero, zero))
    pl.semaphore_wait(heard, 2)
    for c in chips:
        tell(all_heard, beside(*c))
    for n in range(3):
        early[n] = known[n]

    lane = lax.broadcasted_iota(jnp.int32, (rows, nz), 1)
    low = lane < half

    wait_bytes(rs_recv.at[pl.ds(0, no - 1)], recv_sem.at[0])
    s = []
    for p in range(planes):
        total = rs_recv[0, p].astype(F32)
        for o in range(1, no):
            total = total + rs_recv[o, p].astype(F32)
        s.append(total)
    turned = [pltpu.roll(v, half, 1) for v in s]
    for q in range(2):
        stage[:rows, q, :] = jnp.where(low, s[q], turned[q + 2])
        stage[rows:, q, :] = jnp.where(low, turned[q], s[q + 2])
    a_send[...] = stage[...].astype(BF16)

    def slot(j):
        return lax.rem(j, 2) * rows + lax.div(j, 2)

    def all_to_all(source, target, n):
        everyone(me, nd, lambda j: pltpu.make_async_remote_copy(
            source.at[slot(j)], target.at[slot(me)], send_sem.at[n], recv_sem.at[n],
            device_id={"dom": j}, device_id_type=MESH).start())
        target[slot(me)] = source[slot(me)]

    pl.semaphore_wait(all_heard, 3)
    all_to_all(a_send, a_recv, 1)

    @pl.when(top)
    def _():
        upward.start()

    @pl.when(bottom)
    def _():
        downward.start()

    row = mine * rows + lax.div(me, 2)
    column = lax.rem(me, 2) * half + lax.rem(
        lax.broadcasted_iota(jnp.int32, (1, nz), 1), half)
    nx = nd * planes
    kx = folded_square(lax.broadcasted_iota(jnp.int32, (nx, nz), 0), nx)
    ky = folded_square(jnp.full((1, nz), row, jnp.int32), ny)
    weight = (4.0 * np.pi / (nx * ny * nz)) / (kx + (ky + folded_square(column, nz) + screening))
    wide = lax.broadcasted_iota(jnp.int32, (nx, nz), 1) < half

    wait_bytes(a_recv.at[pl.ds(0, nd - 1)], recv_sem.at[1])
    stage[...] = a_recv[...].astype(F32)
    gathered = jnp.concatenate([stage[:, q, :] for q in range(2)], axis=0).astype(BF16)
    size = nx // 2
    first = dot(tx[0, :, :size], gathered) + dot(tx[1, :, :size], gathered)
    second = dot(tx[0, :, size:], gathered) + dot(tx[1, :, size:], gathered)
    modes = jnp.where(
        wide, first + pltpu.roll(second, half, 1), pltpu.roll(first, half, 1) + second)
    modes = split(modes * weight)
    back = dot3((tx[2], tx[3]), modes)
    back = jnp.where(wide[:size], back[:size], back[size:])
    for q in range(2):
        stage[:, q, :] = back[q * nd : (q + 1) * nd]
    b_send[...] = stage[...].astype(BF16)

    all_to_all(b_send, b_recv, 2)
    upward.wait()
    downward.wait()

    def lines(i, carry):
        line = [below[i, p].astype(F32) for p in range(3)]
        line = line + [cur[i, p].astype(F32) for p in range(planes)]
        line = line + [above[i, p].astype(F32) for p in range(3)]
        for p in range(planes):
            value = img[i, p]
            for n, weight in enumerate(side_weights):
                value = value + (-0.5 * weight) * (line[p + 4 + n] + line[p + 2 - n])
            img[i, p] = value
        return carry

    lax.fori_loop(0, count, lines, 0)

    def prepare(p, sums):
        pair = jnp.zeros((ny, nz), F32)
        aged, based, square = pair, pair, pair
        for i in range(count):
            base, weight_o = img[i, p], orb[i, p].astype(F32)
            value, old = cur[i, p].astype(F32), pre[i, p].astype(F32)
            pair = pair + weight_o * value
            aged = aged + weight_o * old
            based = based + weight_o * base
            square = square + weight_o * weight_o
            sums = (
                sums[0] + folded(value * base),
                sums[1] + folded(base * base),
                sums[2] + folded(old * base),
            )
        for n, field in enumerate((pair, aged, 2.0 * based, square)):
            mixed_fields[n, p] = field
        return sums

    based = lax.fori_loop(0, planes, prepare, (zero, zero, zero))
    for n in range(3):
        early[3 + n] = based[n]

    wait_bytes(b_recv.at[pl.ds(0, nd - 1)], recv_sem.at[2])
    stage[...] = b_recv[...].astype(F32)
    for q in range(2):
        even, odd = stage[:rows, q, :], stage[rows:, q, :]
        g_send[q] = jnp.where(low, even, pltpu.roll(odd, half, 1)).astype(BF16)
        g_send[q + 2] = jnp.where(low, pltpu.roll(even, half, 1), odd).astype(BF16)

    for p in range(planes):
        cyclic(mine, no, lambda j: pltpu.make_async_remote_copy(
            g_send.at[p], g_recv.at[mine, p], send_sem.at[3], plane_sem.at[p],
            device_id={"orb": j}, device_id_type=MESH).start())
    g_recv[mine] = g_send[...]

    late = (early[3], early[4], early[5])
    for p in range(0, planes, 2):
        for n in range(2):
            wait_bytes(g_recv.at[pl.ds(0, no - 1), p + n], plane_sem.at[p + n])
        field = across([g_recv[:, p + n].reshape(ny, nz) for n in range(2)])
        field = dot(ty[0], field) + dot(ty[1], field)
        field = dot3(split(stacked(field)), cz)
        for n in range(2):
            part = field[n * ny : (n + 1) * ny]
            potential[p + n] = part
            late = (
                late[0] + folded(mixed_fields[0, p + n] * part),
                late[1] + folded((mixed_fields[2, p + n] + mixed_fields[3, p + n] * part) * part),
                late[2] + folded(mixed_fields[1, p + n] * part),
            )

    ones = lax.broadcasted_iota(jnp.int32, (1, nz), 1)

    def whole(value):
        return jnp.sum(jnp.sum(value, axis=0, keepdims=True), axis=1, keepdims=True)

    packed = jnp.zeros((1, nz), F32)
    for n, value in enumerate((*late, early[0], early[1], early[2])):
        packed = jnp.where(ones == n, whole(value), packed)
    mo_send[...] = packed
    here = mine * 4 + wide_x * 2 + core
    for step in range(no):
        for c in chips + ((0, 0),):
            if step or c != (0, 0):
                pltpu.make_async_remote_copy(
                    mo_send, mo_recv.at[here], send_sem.at[4], recv_sem.at[4],
                    device_id={"dom": beside(*c), "orb": lax.rem(mine + step, no)},
                    device_id_type=MESH).start()
    mo_recv[here] = packed
    wait_bytes(mo_recv.at[pl.ds(0, 4 * no - 1)], recv_sem.at[4])
    packed = jnp.sum(mo_recv[...], axis=0)
    md_send[...] = packed
    for step in sorted(range(1, ring), key=lambda n: abs(2 * n - ring)):
        pltpu.make_async_remote_copy(
            md_send, md_recv.at[depth], send_sem.at[5], recv_sem.at[5],
            device_id={"dom": along(step)}, device_id_type=MESH).start()
    md_recv[depth] = packed
    beta_now = beta[0]

    def ready(n, carry):
        i, p = lax.div(n, planes), lax.rem(n, planes)
        value = img[i, p] + orb[i, p].astype(F32) * potential[p]
        img[i, p] = value - beta_now * pre[i, p].astype(F32)
        return carry

    lax.fori_loop(0, count * planes, ready, 0)
    wait_bytes(md_recv.at[pl.ds(0, ring - 1)], recv_sem.at[5])
    packed = jnp.sum(md_recv[...], axis=0) * (1.0 / (count * no * nx * ny * nz))

    cross, image, older_image, own, mixed, older = [
        jnp.sum(jnp.where(ones == n, packed, 0.0), axis=1, keepdims=True) for n in range(6)
    ]
    squares = image - 2.0 * cross * cross - 2.0 * beta_now * older_image
    squares = squares + cross * cross * own + 2.0 * cross * beta_now * mixed
    squares = squares + beta_now * beta_now * older
    norm = jnp.sqrt(squares + 1e-06)
    inverse = 1.0 / norm
    alpha_out[0] = cross[0, 0]
    norm_out[0] = norm[0, 0]

    def scale(n, carry):
        i, p = lax.div(n, planes), lax.rem(n, planes)
        value = img[i, p] - cross * cur[i, p].astype(F32)
        out[i, p] = (value * inverse).astype(BF16)
        return carry

    lax.fori_loop(0, count * planes, scale, 0)
    wait_bytes(rs_send.at[pl.ds(0, no - 1)], send_sem.at[0])
    wait_bytes(a_send.at[pl.ds(0, nd - 1)], send_sem.at[1])
    wait_bytes(b_send.at[pl.ds(0, nd - 1)], send_sem.at[2])
    wait_bytes(g_recv.at[pl.ds(0, no - 1)], send_sem.at[3])
    wait_bytes(mo_recv.at[pl.ds(0, 4 * no - 1)], send_sem.at[4])
    wait_bytes(md_recv.at[pl.ds(0, ring - 1)], send_sem.at[5])


def emit(*refs):
    copies = [pltpu.make_async_copy(refs[n], refs[n + 3], refs[6].at[n]) for n in range(3)]
    for copy in copies:
        copy.start()
    for copy in copies:
        copy.wait()


def per_device(nd, no, orbitals, energies, local_potential, lanczos, previous, beta):
    count, planes, ny, nz = lanczos.shape
    rows, nx = ny // no, nd * planes
    order = np.array([
        planes * (2 * r + h) + 2 * lane_half + q
        for lane_half in range(2) for q in range(2) for h in range(2) for r in range(rows)
    ])
    cas_x = cas_table(nx)
    t128 = np.stack(high_low(cas_table(nz)) + high_low(side_table(nz, central_weight)))
    ty = np.stack(high_low(cas_table(ny)) + high_low(side_table(ny, 2.0 * central_weight)))
    tx = np.stack(high_low(cas_x[:, order]) + high_low(cas_x[order, :]))
    smem = pl.BlockSpec(memory_space=pltpu.SMEM)
    vmem = pltpu.VMEM
    field = (count, planes, ny, nz)
    dma = pltpu.SemaphoreType.DMA
    results = pl.pallas_call(
        functools.partial(kernel, nd, no),
        out_shape=(
            pltpu.VMEM(field, BF16),
            pltpu.SMEM((1,), F32),
            pltpu.SMEM((1,), F32),
        ),
        in_specs=[pl.BlockSpec(memory_space=pltpu.HBM)] * 9,
        out_specs=(pl.BlockSpec(memory_space=vmem), smem, smem),
        scratch_shapes=[
            vmem(field, BF16), vmem(field[1:], F32), vmem(field, BF16), vmem(field, BF16),
            vmem(t128.shape, BF16), vmem(ty.shape, BF16), vmem(tx.shape, BF16),
            vmem(field, F32),
            vmem((count, 3, ny, nz), BF16), vmem((count, 3, ny, nz), BF16),
            vmem((no, planes, rows, nz), BF16), vmem((no, planes, rows, nz), BF16),
            vmem((nd, 2, nz), BF16), vmem((nd, 2, nz), BF16),
            vmem((nd, 2, nz), BF16), vmem((nd, 2, nz), BF16),
            vmem((planes, rows, nz), BF16), vmem((no, planes, rows, nz), BF16),
            vmem((1, nz), F32), vmem((4 * no, 1, nz), F32),
            vmem((1, nz), F32), vmem((nd // 4, 1, nz), F32),
            vmem((6, 8, nz), F32), vmem((nd, 2, nz), F32),
            vmem((4, *field[1:]), F32), vmem(field[1:], F32),
            pltpu.SMEM((count,), F32), pltpu.SMEM((1,), F32),
            dma((9,)), dma((4,)), dma((6,)), dma((6,)), dma((planes,)),
            pltpu.SemaphoreType.REGULAR(()), pltpu.SemaphoreType.REGULAR(()),
        ],
        compiler_params=pltpu.CompilerParams(collective_id=0, has_side_effects=True),
    )(energies, beta, orbitals, local_potential, lanczos, previous,
      jnp.asarray(t128), jnp.asarray(ty), jnp.asarray(tx))
    return pl.pallas_call(
        emit,
        out_shape=tuple(jax.ShapeDtypeStruct(r.shape, r.dtype) for r in results),
        in_specs=[pl.BlockSpec(memory_space=vmem), smem, smem],
        out_specs=(pl.BlockSpec(memory_space=pltpu.HBM),) * 3,
        scratch_shapes=[dma((3,))],
    )(pltpu.with_memory_space_constraint(results[0], pltpu.VMEM), *results[1:])


def solution(mesh):
    placed = (
        P("orb", "dom", None, None),
        P("orb"),
        P("dom", None, None),
        P("orb", "dom", None, None),
        P("orb", "dom", None, None),
        P(),
    )
    return jax.shard_map(
        functools.partial(per_device, mesh.shape["dom"], mesh.shape["orb"]),
        mesh=mesh,
        in_specs=placed,
        out_specs=(P("orb", "dom", None, None), P(), P()),
        check_vma=False,
    )
```

```python
import functools

import jax
import jax.numpy as jnp
import ml_dtypes
import numpy as np
from jax import lax
from jax.experimental import pallas as pl
from jax.experimental.pallas import tpu as pltpu
from jax.sharding import PartitionSpec as P

side_weights = (1.5, -0.15, 1.0 / 90.0)
central_weight = -49.0 / 18.0
screening = 1.0 / 64.0
MESH = pl.DeviceIdType.MESH
F32 = jnp.float32
BF16 = jnp.bfloat16


def cas_table(length):
    position = np.arange(length)
    angle = 2.0 * np.pi / length * (position[:, None] * position[None, :] % length)
    return np.cos(angle) + np.sin(angle)


def side_table(length, center):
    table = center * np.eye(length)
    for offset, weight in enumerate(side_weights):
        for shift in (offset + 1, -offset - 1):
            table = table + weight * np.roll(np.eye(length), shift, 0)
    return -0.5 * table


def high_low(table):
    high = table.astype(np.float32).astype(ml_dtypes.bfloat16)
    low = (table - high.astype(np.float64)).astype(np.float32).astype(ml_dtypes.bfloat16)
    return [high, low]


def split(value):
    high = value.astype(BF16)
    return high, (value - high.astype(F32)).astype(BF16)


def dot(a, b):
    return jnp.dot(a, b, preferred_element_type=F32)


def dot3(a, b):
    return dot(a[0], b[0]) + (dot(a[0], b[1]) + dot(a[1], b[0]))


def folded_square(position, length):
    folded = jnp.minimum(position, length - position).astype(F32) * (2.0 * np.pi / length)
    return folded * folded


def everyone(me, size, action):
    quarter = size // 4
    around = lambda offset: action(lax.rem(me + offset, size))
    around(quarter)
    around(3 * quarter)

    block = 3 if (quarter - 1) % 3 == 0 else 1

    def nearer(n, carry):
        for part in range(block):
            step = n * block + part + 1
            around(quarter + step)
            around(quarter - step)
            around(3 * quarter + step)
            around(3 * quarter - step)
        return carry

    lax.fori_loop(0, (quarter - 1) // block, nearer, 0)
    around(2 * quarter)


def far_first(start, size):
    return sorted(range(start, size), key=lambda n: abs(2 * n - size))


def cyclic(me, size, action):
    for step in far_first(1, size):
        action(lax.rem(me + step, size))


def wait_bytes(ref, sem):
    pltpu.make_async_copy(ref, ref, sem).wait()


def kernel(
    nd, no, energies_hbm, beta_hbm, orb_hbm, loc_hbm, cur_hbm, pre_hbm, t128_hbm, ty_hbm, tx_hbm,
    out, alpha_out, norm_out,
    orb, loc, cur, pre, t128, ty, tx, img, below, above,
    rs_send, rs_recv, a_send, a_recv, b_send, b_recv, g_send, g_recv,
    mo_send, mo_recv, md_send, md_recv, early, stage, mixed_fields, potential, energies, beta,
    load_sem, near_sem, send_sem, recv_sem, plane_sem, heard, all_heard,
):
    me = lax.axis_index("dom")
    mine = lax.axis_index("orb")
    count, planes, ny, nz = cur.shape
    rows = ny // no
    half = nz // 2
    loads = [
        pltpu.make_async_copy(s, d, load_sem.at[n])
        for n, (s, d) in enumerate((
            (cur_hbm, cur), (orb_hbm, orb), (t128_hbm, t128), (ty_hbm, ty),
            (pre_hbm, pre), (loc_hbm, loc), (tx_hbm, tx),
            (energies_hbm, energies), (beta_hbm, beta),
        ))
    ]
    for load in loads[:4]:
        load.start()
    ring = nd // 4
    core = lax.rem(me, 2)
    wide_x = lax.div(me, nd // 2)
    depth = lax.rem(lax.div(me, 2), ring)

    def along(offset):
        return wide_x * (nd // 2) + lax.rem(depth + offset + ring, ring) * 2 + core

    def beside(a, b):
        return lax.rem(wide_x + a, 2) * (nd // 2) + depth * 2 + lax.rem(core + b, 2)

    outer = lax.rem(me + 2 * core - 1 + nd, nd)
    chips = ((1, 1), (1, 0), (0, 1))

    def tell(sem, j):
        pl.semaphore_signal(sem, inc=1, device_id={"dom": j}, device_id_type=MESH)

    barrier = pltpu.get_barrier_semaphore()
    cyclic(mine, no, lambda j: pl.semaphore_signal(
        barrier, inc=1, device_id={"orb": j}, device_id_type=MESH))
    near = ring // 4
    for step in range(near, 0, -1):
        tell(barrier, along(step))
        tell(barrier, along(-step))
    for j in [beside(*c) for c in chips] + [outer]:
        tell(barrier, j)

    for load in loads[:4]:
        load.wait()
    for load in loads[4:]:
        load.start()
    cz = (t128[0], t128[1])

    def across(fields):
        return jnp.concatenate(fields, axis=1)

    def stacked(field):
        return jnp.concatenate([field[:, :nz], field[:, nz:]], axis=0)

    def forward(p):
        fields = []
        for n in range(2):
            field = jnp.zeros((ny, nz), F32)
            for i in range(count):
                field = field + orb[i, p + n].astype(F32) * cur[i, p + n].astype(F32)
            fields.append(field)
        field = dot3(split(jnp.concatenate(fields, axis=0)), cz)
        field = dot3((ty[0], ty[1]), split(across([field[:ny], field[ny:]])))
        for n in range(2):
            part = field[:, n * nz : (n + 1) * nz]
            rs_send[:, p + n] = part.reshape(no, rows, nz).astype(BF16)

    def scatter(p):
        cyclic(mine, no, lambda j: pltpu.make_async_remote_copy(
            rs_send.at[j, p], rs_recv.at[mine, p], send_sem.at[0], recv_sem.at[0],
            device_id={"orb": j}, device_id_type=MESH).start())

    for p in range(0, planes, 2):
        forward(p)
        if p == 0:
            pl.semaphore_wait(barrier, no + 3 + 2 * near)
            tell(heard, along(near))
            tell(heard, along(-near))
        scatter(p)
        scatter(p + 1)
    upward = pltpu.make_async_remote_copy(
        cur.at[:, pl.ds(planes - 3, 3)], below, near_sem.at[0], near_sem.at[1],
        device_id={"dom": lax.rem(me + 1, nd)}, device_id_type=MESH)
    downward = pltpu.make_async_remote_copy(
        cur.at[:, pl.ds(0, 3)], above, near_sem.at[2], near_sem.at[3],
        device_id={"dom": lax.rem(me + nd - 1, nd)}, device_id_type=MESH)
    turn = nd // 2
    top = lax.rem(me, turn) == turn - 1
    bottom = lax.rem(me, turn) == 0

    @pl.when(jnp.logical_not(top))
    def _():
        upward.start()

    @pl.when(jnp.logical_not(bottom))
    def _():
        downward.start()

    rs_recv[mine] = rs_send[mine]

    for load in loads[4:]:
        load.wait()

    def folded(value):
        return jnp.sum(value.reshape(ny // 8, 8, nz), axis=0)

    def local(n, sums):
        i, p = lax.div(n, planes), lax.rem(n, planes)
        here = cur[i, p]
        value = here.astype(F32)
        old = pre[i, p].astype(F32)
        near = dot(ty[2], here) + dot(ty[3], here)
        near = near + dot(here, t128[2]) + dot(here, t128[3])
        img[i, p] = near + (loc[p] - energies[i]) * value
        return (
            sums[0] + folded(value * value),
            sums[1] + folded(value * old),
            sums[2] + folded(old * old),
        )

    zero = jnp.zeros((8, nz), F32)
    known = lax.fori_loop(0, count * planes, local, (zero, zero, zero))
    pl.semaphore_wait(heard, 2)
    for c in chips:
        tell(all_heard, beside(*c))
    for n in range(3):
        early[n] = known[n]

    lane = lax.broadcasted_iota(jnp.int32, (rows, nz), 1)
    low = lane < half

    wait_bytes(rs_recv.at[pl.ds(0, no - 1)], recv_sem.at[0])
    s = []
    for p in range(planes):
        total = rs_recv[0, p].astype(F32)
        for o in range(1, no):
            total = total + rs_recv[o, p].astype(F32)
        s.append(total)
    turned = [pltpu.roll(v, half, 1) for v in s]
    for q in range(2):
        stage[:rows, q, :] = jnp.where(low, s[q], turned[q + 2])
        stage[rows:, q, :] = jnp.where(low, turned[q], s[q + 2])
    a_send[...] = stage[...].astype(BF16)

    def slot(j):
        return lax.rem(j, 2) * rows + lax.div(j, 2)

    def all_to_all(source, target, n):
        everyone(me, nd, lambda j: pltpu.make_async_remote_copy(
            source.at[slot(j)], target.at[slot(me)], send_sem.at[n], recv_sem.at[n],
            device_id={"dom": j}, device_id_type=MESH).start())
        target[slot(me)] = source[slot(me)]

    pl.semaphore_wait(all_heard, 3)
    all_to_all(a_send, a_recv, 1)

    @pl.when(top)
    def _():
        upward.start()

    @pl.when(bottom)
    def _():
        downward.start()

    row = mine * rows + lax.div(me, 2)
    column = lax.rem(me, 2) * half + lax.rem(
        lax.broadcasted_iota(jnp.int32, (1, nz), 1), half)
    nx = nd * planes
    kx = folded_square(lax.broadcasted_iota(jnp.int32, (nx, nz), 0), nx)
    ky = folded_square(jnp.full((1, nz), row, jnp.int32), ny)
    weight = (4.0 * np.pi / (nx * ny * nz)) / (kx + (ky + folded_square(column, nz) + screening))
    wide = lax.broadcasted_iota(jnp.int32, (nx, nz), 1) < half

    wait_bytes(a_recv.at[pl.ds(0, nd - 1)], recv_sem.at[1])
    stage[...] = a_recv[...].astype(F32)
    gathered = jnp.concatenate([stage[:, q, :] for q in range(2)], axis=0).astype(BF16)
    size = nx // 2
    first = dot(tx[0, :, :size], gathered) + dot(tx[1, :, :size], gathered)
    second = dot(tx[0, :, size:], gathered) + dot(tx[1, :, size:], gathered)
    modes = jnp.where(
        wide, first + pltpu.roll(second, half, 1), pltpu.roll(first, half, 1) + second)
    modes = split(modes * weight)
    back = dot3((tx[2], tx[3]), modes)
    back = jnp.where(wide[:size], back[:size], back[size:])
    for q in range(2):
        stage[:, q, :] = back[q * nd : (q + 1) * nd]
    b_send[...] = stage[...].astype(BF16)

    all_to_all(b_send, b_recv, 2)
    upward.wait()
    downward.wait()

    def lines(i, carry):
        line = [below[i, p].astype(F32) for p in range(3)]
        line = line + [cur[i, p].astype(F32) for p in range(planes)]
        line = line + [above[i, p].astype(F32) for p in range(3)]
        for p in range(planes):
            value = img[i, p]
            for n, weight in enumerate(side_weights):
                value = value + (-0.5 * weight) * (line[p + 4 + n] + line[p + 2 - n])
            img[i, p] = value
        return carry

    lax.fori_loop(0, count, lines, 0)

    def prepare(p, sums):
        pair = jnp.zeros((ny, nz), F32)
        aged, based, square = pair, pair, pair
        for i in range(count):
            base, weight_o = img[i, p], orb[i, p].astype(F32)
            value, old = cur[i, p].astype(F32), pre[i, p].astype(F32)
            pair = pair + weight_o * value
            aged = aged + weight_o * old
            based = based + weight_o * base
            square = square + weight_o * weight_o
            sums = (
                sums[0] + folded(value * base),
                sums[1] + folded(base * base),
                sums[2] + folded(old * base),
            )
        for n, field in enumerate((pair, aged, 2.0 * based, square)):
            mixed_fields[n, p] = field
        return sums

    based = lax.fori_loop(0, planes, prepare, (zero, zero, zero))
    for n in range(3):
        early[3 + n] = based[n]

    wait_bytes(b_recv.at[pl.ds(0, nd - 1)], recv_sem.at[2])
    stage[...] = b_recv[...].astype(F32)
    for q in range(2):
        even, odd = stage[:rows, q, :], stage[rows:, q, :]
        g_send[q] = jnp.where(low, even, pltpu.roll(odd, half, 1)).astype(BF16)
        g_send[q + 2] = jnp.where(low, pltpu.roll(even, half, 1), odd).astype(BF16)

    for p in range(planes):
        cyclic(mine, no, lambda j: pltpu.make_async_remote_copy(
            g_send.at[p], g_recv.at[mine, p], send_sem.at[3], plane_sem.at[p],
            device_id={"orb": j}, device_id_type=MESH).start())
    g_recv[mine] = g_send[...]

    late = (early[3], early[4], early[5])
    for p in range(0, planes, 2):
        for n in range(2):
            wait_bytes(g_recv.at[pl.ds(0, no - 1), p + n], plane_sem.at[p + n])
        field = across([g_recv[:, p + n].reshape(ny, nz) for n in range(2)])
        field = dot(ty[0], field) + dot(ty[1], field)
        field = dot3(split(stacked(field)), cz)
        for n in range(2):
            part = field[n * ny : (n + 1) * ny]
            potential[p + n] = part
            late = (
                late[0] + folded(mixed_fields[0, p + n] * part),
                late[1] + folded((mixed_fields[2, p + n] + mixed_fields[3, p + n] * part) * part),
                late[2] + folded(mixed_fields[1, p + n] * part),
            )

    ones = lax.broadcasted_iota(jnp.int32, (1, nz), 1)

    def whole(value):
        return jnp.sum(jnp.sum(value, axis=0, keepdims=True), axis=1, keepdims=True)

    packed = jnp.zeros((1, nz), F32)
    for n, value in enumerate((*late, early[0], early[1], early[2])):
        packed = jnp.where(ones == n, whole(value), packed)
    mo_send[...] = packed
    here = mine * 4 + wide_x * 2 + core
    for step in far_first(0, no):
        for c in chips + ((0, 0),):
            if step or c != (0, 0):
                pltpu.make_async_remote_copy(
                    mo_send, mo_recv.at[here], send_sem.at[4], recv_sem.at[4],
                    device_id={"dom": beside(*c), "orb": lax.rem(mine + step, no)},
                    device_id_type=MESH).start()
    mo_recv[here] = packed
    wait_bytes(mo_recv.at[pl.ds(0, 4 * no - 1)], recv_sem.at[4])
    packed = jnp.sum(mo_recv[...], axis=0)
    md_send[...] = packed
    for step in far_first(1, ring):
        pltpu.make_async_remote_copy(
            md_send, md_recv.at[depth], send_sem.at[5], recv_sem.at[5],
            device_id={"dom": along(step)}, device_id_type=MESH).start()
    md_recv[depth] = packed
    beta_now = beta[0]

    def ready(n, carry):
        i, p = lax.div(n, planes), lax.rem(n, planes)
        value = img[i, p] + orb[i, p].astype(F32) * potential[p]
        img[i, p] = value - beta_now * pre[i, p].astype(F32)
        return carry

    lax.fori_loop(0, count * planes, ready, 0)
    wait_bytes(md_recv.at[pl.ds(0, ring - 1)], recv_sem.at[5])
    packed = jnp.sum(md_recv[...], axis=0) * (1.0 / (count * no * nx * ny * nz))

    cross, image, older_image, own, mixed, older = [
        jnp.sum(jnp.where(ones == n, packed, 0.0), axis=1, keepdims=True) for n in range(6)
    ]
    squares = image - 2.0 * cross * cross - 2.0 * beta_now * older_image
    squares = squares + cross * cross * own + 2.0 * cross * beta_now * mixed
    squares = squares + beta_now * beta_now * older
    norm = jnp.sqrt(squares + 1e-06)
    inverse = 1.0 / norm
    alpha_out[0] = cross[0, 0]
    norm_out[0] = norm[0, 0]

    def scale(n, carry):
        i, p = lax.div(n, planes), lax.rem(n, planes)
        value = img[i, p] - cross * cur[i, p].astype(F32)
        out[i, p] = (value * inverse).astype(BF16)
        return carry

    lax.fori_loop(0, count * planes, scale, 0)
    wait_bytes(rs_send.at[pl.ds(0, no - 1)], send_sem.at[0])
    wait_bytes(a_send.at[pl.ds(0, nd - 1)], send_sem.at[1])
    wait_bytes(b_send.at[pl.ds(0, nd - 1)], send_sem.at[2])
    wait_bytes(g_recv.at[pl.ds(0, no - 1)], send_sem.at[3])
    wait_bytes(mo_recv.at[pl.ds(0, 4 * no - 1)], send_sem.at[4])
    wait_bytes(md_recv.at[pl.ds(0, ring - 1)], send_sem.at[5])


def emit(*refs):
    copies = [pltpu.make_async_copy(refs[n], refs[n + 3], refs[6].at[n]) for n in range(3)]
    for copy in copies:
        copy.start()
    for copy in copies:
        copy.wait()


def per_device(nd, no, orbitals, energies, local_potential, lanczos, previous, beta):
    count, planes, ny, nz = lanczos.shape
    rows, nx = ny // no, nd * planes
    order = np.array([
        planes * (2 * r + h) + 2 * lane_half + q
        for lane_half in range(2) for q in range(2) for h in range(2) for r in range(rows)
    ])
    cas_x = cas_table(nx)
    t128 = np.stack(high_low(cas_table(nz)) + high_low(side_table(nz, central_weight)))
    ty = np.stack(high_low(cas_table(ny)) + high_low(side_table(ny, 2.0 * central_weight)))
    tx = np.stack(high_low(cas_x[:, order]) + high_low(cas_x[order, :]))
    smem = pl.BlockSpec(memory_space=pltpu.SMEM)
    vmem = pltpu.VMEM
    field = (count, planes, ny, nz)
    dma = pltpu.SemaphoreType.DMA
    results = pl.pallas_call(
        functools.partial(kernel, nd, no),
        out_shape=(
            pltpu.VMEM(field, BF16),
            pltpu.SMEM((1,), F32),
            pltpu.SMEM((1,), F32),
        ),
        in_specs=[pl.BlockSpec(memory_space=pltpu.HBM)] * 9,
        out_specs=(pl.BlockSpec(memory_space=vmem), smem, smem),
        scratch_shapes=[
            vmem(field, BF16), vmem(field[1:], F32), vmem(field, BF16), vmem(field, BF16),
            vmem(t128.shape, BF16), vmem(ty.shape, BF16), vmem(tx.shape, BF16),
            vmem(field, F32),
            vmem((count, 3, ny, nz), BF16), vmem((count, 3, ny, nz), BF16),
            vmem((no, planes, rows, nz), BF16), vmem((no, planes, rows, nz), BF16),
            vmem((nd, 2, nz), BF16), vmem((nd, 2, nz), BF16),
            vmem((nd, 2, nz), BF16), vmem((nd, 2, nz), BF16),
            vmem((planes, rows, nz), BF16), vmem((no, planes, rows, nz), BF16),
            vmem((1, nz), F32), vmem((4 * no, 1, nz), F32),
            vmem((1, nz), F32), vmem((nd // 4, 1, nz), F32),
            vmem((6, 8, nz), F32), vmem((nd, 2, nz), F32),
            vmem((4, *field[1:]), F32), vmem(field[1:], F32),
            pltpu.SMEM((count,), F32), pltpu.SMEM((1,), F32),
            dma((9,)), dma((4,)), dma((6,)), dma((6,)), dma((planes,)),
            pltpu.SemaphoreType.REGULAR(()), pltpu.SemaphoreType.REGULAR(()),
        ],
        compiler_params=pltpu.CompilerParams(collective_id=0, has_side_effects=True),
    )(energies, beta, orbitals, local_potential, lanczos, previous,
      jnp.asarray(t128), jnp.asarray(ty), jnp.asarray(tx))
    return pl.pallas_call(
        emit,
        out_shape=tuple(jax.ShapeDtypeStruct(r.shape, r.dtype) for r in results),
        in_specs=[pl.BlockSpec(memory_space=vmem), smem, smem],
        out_specs=(pl.BlockSpec(memory_space=pltpu.HBM),) * 3,
        scratch_shapes=[dma((3,))],
    )(pltpu.with_memory_space_constraint(results[0], pltpu.VMEM), *results[1:])


def solution(mesh):
    placed = (
        P("orb", "dom", None, None),
        P("orb"),
        P("dom", None, None),
        P("orb", "dom", None, None),
        P("orb", "dom", None, None),
        P(),
    )
    return jax.shard_map(
        functools.partial(per_device, mesh.shape["dom"], mesh.shape["orb"]),
        mesh=mesh,
        in_specs=placed,
        out_specs=(P("orb", "dom", None, None), P(), P()),
        check_vma=False,
    )
```
